64 devices in a mesh: dp: 4 (over x, y), cp: 16 (over z, core).
Axes of the slice: x: 2, y: 2, z: 8, core: 2. Of those that a mesh axis runs over, the one named last changes fastest.
The devices are a block of a 4x4x8 slice.
Arguments:
- x_norm: bfloat16 [4096, 2048], P(('dp', 'cp')), parts along dimension 0
- y_grad: bfloat16 [4096, 2048], P(('dp', 'cp')), parts along dimension 0
- w_q: bfloat16 [2048, 16, 192], replicated
- w_dkv: bfloat16 [2048, 512], replicated
- g_kv: bfloat16 [512], replicated
- w_kr: bfloat16 [2048, 64], replicated
- w_uk: bfloat16 [512, 16, 128], replicated
- w_uv: bfloat16 [512, 16, 128], replicated
- w_o: bfloat16 [16, 128, 2048], replicated
Outputs:
- output 1: bfloat16 [4096, 2048], P(('dp', 'cp')), parts along dimension 0
- output 2: bfloat16 [4096, 2048], P(('dp', 'cp')), parts along dimension 0
- output 3: float32 [8192, 16, 192], P('dp'), parts along dimension 0
- output 4: float32 [8192, 512], P('dp'), parts along dimension 0
- output 5: float32 [2048], P('dp'), parts along dimension 0
- output 6: float32 [8192, 64], P('dp'), parts along dimension 0
- output 7: float32 [2048, 16, 128], P('dp'), parts along dimension 0
- output 8: float32 [2048, 16, 128], P('dp'), parts along dimension 0
- output 9: float32 [64, 128, 2048], P('dp'), parts along dimension 0
There are 4 independent parts. The reference program is written for one: setup_inputs(seed, part) draws one part's arguments, and reference() takes and returns one part's arrays. A program takes and returns all parts, laid end to end along the dimension named above; an argument that names none is the same for every part.
All inputs are finite; a program needn't handle non-finite values.
Results may differ from the reference program's by a relative error of at most 0.0156227.
Values are sent between devices in bfloat16 or wider.
A program may use at most 768 MiB of HBM per device.

```python
import jax
import jax.numpy as jnp
from jax import lax

D = 2048
HEADS = 16
KV_RANK = 512
NOPE = 128
ROPE = 64
VDIM = 128
SEQ = 1024
QBLK = 64
QK_DIM = NOPE + ROPE
ROPE_THETA = 10000.0
NORM_EPS = 1e-6


def setup_inputs(seed: int = 0, part: int = 0) -> dict:
    part_key = jax.random.fold_in(jax.random.key(seed), part)
    key_x, key_gy = jax.random.split(part_key, 2)
    weight_keys = jax.random.split(jax.random.key(seed + 1), 7)
    o_scale = (HEADS * VDIM) ** -0.5 * SEQ ** 0.5 / 6.0
    x_norm = jax.random.normal(key_x, (SEQ, D), jnp.float32)
    y_grad = jax.random.normal(key_gy, (SEQ, D), jnp.float32)
    w_q = jax.random.normal(weight_keys[0], (D, HEADS, QK_DIM), jnp.float32) * (1.5 * D ** -0.5)
    w_dkv = jax.random.normal(weight_keys[1], (D, KV_RANK), jnp.float32) * D ** -0.5
    g_kv = 1.0 + 0.3 * jax.random.normal(weight_keys[2], (KV_RANK,), jnp.float32)
    w_kr = jax.random.normal(weight_keys[3], (D, ROPE), jnp.float32) * D ** -0.5
    w_uk = jax.random.normal(weight_keys[4], (KV_RANK, HEADS, NOPE), jnp.float32) * KV_RANK ** -0.5
    w_uv = jax.random.normal(weight_keys[5], (KV_RANK, HEADS, VDIM), jnp.float32) * KV_RANK ** -0.5
    w_o = jax.random.normal(weight_keys[6], (HEADS, VDIM, D), jnp.float32) * o_scale
    return {'x_norm': x_norm.astype(jnp.bfloat16), 'y_grad': y_grad.astype(jnp.bfloat16), 'w_q': w_q.astype(jnp.bfloat16), 'w_dkv': w_dkv.astype(jnp.bfloat16), 'g_kv': g_kv.astype(jnp.bfloat16), 'w_kr': w_kr.astype(jnp.bfloat16), 'w_uk': w_uk.astype(jnp.bfloat16), 'w_uv': w_uv.astype(jnp.bfloat16), 'w_o': w_o.astype(jnp.bfloat16)}


def bf16_straight(t_in):
    return t_in + lax.stop_gradient(t_in.astype(jnp.bfloat16).astype(jnp.float32) - t_in)


def rope_apply(t_in, cos_t, sin_t):
    half_dim = ROPE // 2
    first_half = t_in[..., :half_dim]
    second_half = t_in[..., half_dim:]
    return jnp.concatenate([first_half * cos_t - second_half * sin_t, second_half * cos_t + first_half * sin_t], axis=-1)


def attention_forward(x_in, w_q, w_dkv, g_kv, w_kr, w_uk, w_uv, w_o):
    inv_freq = ROPE_THETA ** (-(jnp.arange(ROPE // 2, dtype=jnp.float32) * 2.0 / ROPE))
    angles = jnp.arange(SEQ, dtype=jnp.float32)[:, None] * inv_freq[None, :]
    cos_t = jnp.cos(angles)
    sin_t = jnp.sin(angles)
    q_full = jnp.einsum('td,dhe->the', x_in, w_q)
    q_nope = bf16_straight(q_full[..., :NOPE])
    q_rope = bf16_straight(rope_apply(q_full[..., NOPE:], cos_t[:, None, :], sin_t[:, None, :]))
    c_raw = jnp.dot(x_in, w_dkv)
    inv_rms = lax.rsqrt(jnp.mean(c_raw * c_raw, axis=-1, keepdims=True) + NORM_EPS)
    latent = bf16_straight(c_raw * inv_rms * g_kv)
    k_rope = bf16_straight(rope_apply(jnp.dot(x_in, w_kr), cos_t, sin_t))
    k_nope = bf16_straight(jnp.einsum('tc,chn->thn', latent, w_uk))
    values = bf16_straight(jnp.einsum('tc,chv->thv', latent, w_uv))
    attn_scale = QK_DIM ** -0.5
    key_pos = jnp.arange(SEQ)

    def block_attn(block_args):
        qn_blk, qr_blk, blk_start = block_args
        scores = (jnp.einsum('qhn,khn->hqk', qn_blk, k_nope) + jnp.einsum('qhr,kr->hqk', qr_blk, k_rope)) * attn_scale
        causal = (blk_start + jnp.arange(QBLK))[:, None] >= key_pos[None, :]
        scores = jnp.where(causal[None], scores, -1e30)
        return jnp.einsum('hqk,khv->qhv', jax.nn.softmax(scores, axis=-1), values)

    num_blocks = SEQ // QBLK
    attn = lax.map(jax.checkpoint(block_attn), (q_nope.reshape(num_blocks, QBLK, HEADS, NOPE), q_rope.reshape(num_blocks, QBLK, HEADS, ROPE), jnp.arange(num_blocks) * QBLK))
    attn = bf16_straight(attn.reshape(SEQ, HEADS, VDIM))
    return jnp.einsum('thv,hvd->td', attn, w_o)


def reference(x_norm, y_grad, w_q, w_dkv, g_kv, w_kr, w_uk, w_uv, w_o):
    y_full, pullback = jax.vjp(attention_forward, x_norm.astype(jnp.float32), w_q.astype(jnp.float32), w_dkv.astype(jnp.float32), g_kv.astype(jnp.float32), w_kr.astype(jnp.float32), w_uk.astype(jnp.float32), w_uv.astype(jnp.float32), w_o.astype(jnp.float32))
    cotangents = pullback(y_grad.astype(jnp.float32))
    return (y_full.astype(jnp.bfloat16), cotangents[0].astype(jnp.bfloat16), cotangents[1], cotangents[2], cotangents[3], cotangents[4], cotangents[5], cotangents[6], cotangents[7])
```

```python
import functools

import jax
import jax.numpy as jnp
from jax import lax
from jax.experimental import pallas as pl
from jax.experimental.pallas import tpu as pltpu
from jax.sharding import PartitionSpec as P

ROPE_THETA = 10000.0
NORM_EPS = 1e-6
QBLK = 256
MASKED = -1e30
F32 = jnp.float32
BF16 = jnp.bfloat16
NN = (((1,), (0,)), ((), ()))
NT = (((1,), (1,)), ((), ()))


def mm(lhs, rhs, dims=NN):
    return lax.dot_general(lhs, rhs, dims, preferred_element_type=F32)


def gather_kernel(n_chips, x_ref, gy_ref, xo_ref, gyo_ref, up_send, up_recv, dn_send, dn_recv, pr_send, pr_recv, own_sem):
    me = lax.axis_index('cp')
    core = lax.rem(me, 2)
    chip = lax.div(me, 2)
    up_dev = lax.rem(chip + 1, n_chips) * 2 + core
    dn_dev = lax.rem(chip + n_chips - 1, n_chips) * 2 + core
    partner = chip * 2 + 1 - core
    rows = x_ref.shape[0]
    part = rows // 2

    barrier = pltpu.get_barrier_semaphore()
    for peer in (up_dev, dn_dev, partner):
        pl.semaphore_signal(barrier, inc=1, device_id={'cp': peer}, device_id_type=pl.DeviceIdType.MESH)
    pl.semaphore_wait(barrier, 3)

    half = n_chips // 2
    hops = ((half, half - 1), (half - 1, half))
    sent = []
    recv_pr = []
    local = []

    def block(out, chip_of, part_idx):
        start = pl.multiple_of((chip_of * 2 + core) * rows + part_idx * part, part)
        return out.at[pl.ds(start, part), :]

    def to_partner(arr, slot, part_idx, out, chip_of, src=None):
        dst = block(out, chip_of, part_idx)
        copy = pltpu.make_async_remote_copy(src_ref=dst if src is None else src, dst_ref=dst, send_sem=pr_send.at[arr, slot, part_idx], recv_sem=pr_recv.at[arr, slot, part_idx], device_id={'cp': partner}, device_id_type=pl.DeviceIdType.MESH)
        copy.start()
        sent.append(copy)
        recv_pr.append(copy)

    def ring(arr, hop, direction, part_idx, out, src=None):
        sends, recvs = (up_send, up_recv) if direction == 0 else (dn_send, dn_recv)
        origin = lax.rem(chip + (n_chips - hop if direction == 0 else hop), n_chips)
        dst = block(out, origin, part_idx)
        copy = pltpu.make_async_remote_copy(src_ref=dst if src is None else src, dst_ref=dst, send_sem=sends.at[arr, hop, part_idx], recv_sem=recvs.at[arr, hop, part_idx], device_id={'cp': up_dev if direction == 0 else dn_dev}, device_id_type=pl.DeviceIdType.MESH)
        copy.start()
        sent.append(copy)
        return copy

    arrays = ((x_ref, xo_ref), (gy_ref, gyo_ref))
    inflight = {}
    for arr, (src, out) in enumerate(arrays):
        for p in range(2):
            piece = src.at[pl.ds(p * part, part), :]
            for d in range(2):
                inflight[arr, 0, d, p] = ring(arr, 0, d, p, out, piece)
        if arr == 0:
            for a2, (s2, o2) in enumerate(arrays):
                for p in range(2):
                    to_partner(a2, 0, p, o2, chip, s2.at[pl.ds(p * part, part), :])
                own = pltpu.make_async_copy(s2, o2.at[pl.ds(pl.multiple_of(me * rows, rows), rows), :], own_sem.at[a2])
                own.start()
                local.append(own)
        for hop in range(1, half + 1):
            for p in range(2):
                for d in range(2):
                    if hop > hops[d][p]:
                        continue
                    inflight[arr, hop - 1, d, p].wait_recv()
                    if hop < hops[d][p]:
                        inflight[arr, hop, d, p] = ring(arr, hop, d, p, out)
                    origin = lax.rem(chip + (n_chips - hop if d == 0 else hop), n_chips)
                    slot = hop if d == 0 else n_chips - hop
                    to_partner(arr, slot, p, out, origin)
    for copy in recv_pr:
        copy.wait_recv()
    for copy in sent:
        copy.wait_send()
    for copy in local:
        copy.wait()


def gather_rows(x_loc, gy_loc, n_dev):
    rows, width = x_loc.shape
    n_chips = n_dev // 2
    half = n_chips // 2
    full = jax.ShapeDtypeStruct((rows * n_dev, width), x_loc.dtype)
    dma = pltpu.SemaphoreType.DMA
    return pl.pallas_call(
        functools.partial(gather_kernel, n_chips),
        out_shape=(full, full),
        in_specs=[pl.BlockSpec(memory_space=pl.ANY)] * 2,
        out_specs=[pl.BlockSpec(memory_space=pl.ANY)] * 2,
        scratch_shapes=[dma((2, half, 2)), dma((2, half, 2)), dma((2, half, 2)), dma((2, half, 2)), dma((2, n_chips, 2)), dma((2, n_chips, 2)), dma((2,))],
        compiler_params=pltpu.CompilerParams(collective_id=0, has_side_effects=True),
        name='gather_rows',
    )(x_loc, gy_loc)


def swap_halves(t):
    return pltpu.roll(t, 32, 1) + pltpu.roll(t, 96, 1)


def attention_kernel(scale, x_ref, gy_ref, lat_ref, kr_ref, cos_ref, sin_ref, cost_ref, sint_ref, wq_ref, wuk_ref, wuv_ref, wo_ref,
                     ot_out, dqt_out, dk_out, dv_out, dkr_out,
                     q_s, k_s, kt_s, v_s, vt_s, do_s, dot_s, dk_acc, dv_acc, dkr_acc, ot_st, dqt_st, dk_st, dv_st,
                     loc_sem, snd_sem, rcv_sem, kr_sem):
    g = pl.program_id(0)
    n_pairs = pl.num_programs(0)
    me = lax.axis_index('cp')
    core = lax.rem(me, 2)
    partner = me + 1 - 2 * core
    seq = x_ref.shape[0]
    nope = 128
    qk = wq_ref.shape[0] // 2
    slot = lax.rem(g, 2)

    def copies(step, slot_of):
        pair = core * n_pairs + step
        at = lambda ref, size, axis: ref.at[pl.ds(pl.multiple_of(pair * size, size), size), :] if axis == 0 else ref.at[:, pl.ds(pl.multiple_of(pair * size, size), size)]
        regions = ((ot_st.at[slot_of], at(ot_out, 2 * nope, 0)), (dqt_st.at[slot_of], at(dqt_out, 2 * qk, 0)), (dk_st.at[slot_of], at(dk_out, 2 * nope, 1)), (dv_st.at[slot_of], at(dv_out, 2 * nope, 1)))
        local, remote = [], []
        for idx, (src, dst) in enumerate(regions):
            local.append(pltpu.make_async_copy(src, dst, loc_sem.at[slot_of, idx]))
            remote.append(pltpu.make_async_remote_copy(src_ref=src, dst_ref=dst, send_sem=snd_sem.at[slot_of, idx], recv_sem=rcv_sem.at[step, idx], device_id={'cp': partner}, device_id_type=pl.DeviceIdType.MESH))
        return local, remote

    @pl.when(g == 0)
    def _():
        barrier = pltpu.get_barrier_semaphore()
        pl.semaphore_signal(barrier, inc=1, device_id={'cp': partner}, device_id_type=pl.DeviceIdType.MESH)
        pl.semaphore_wait(barrier, 1)
        dkr_acc[...] = jnp.zeros_like(dkr_acc)

    @pl.when(g >= 2)
    def _():
        local, remote = copies(g - 2, slot)
        for copy in local:
            copy.wait()
        for copy in remote:
            copy.wait_send()

    do_all = mm(gy_ref[...], wo_ref[...], NT).astype(BF16)
    do_s[...] = do_all
    dot_s[...] = do_all.T
    pad = jnp.zeros((256 - qk, wq_ref.shape[1]), BF16)
    row_id = lax.broadcasted_iota(jnp.int32, (QBLK, QBLK), 0)
    col_id = lax.broadcasted_iota(jnp.int32, (QBLK, QBLK), 1)
    causal = row_id <= col_id
    n_blk = seq // QBLK
    for hh in range(2):
        w_ext = jnp.concatenate([wq_ref[hh * qk:(hh + 1) * qk, :], pad], axis=0)
        q_raw = mm(x_ref[...], w_ext, NT)
        q_s[:, :nope] = q_raw[:, :nope].astype(BF16)
        rope = q_raw[:, nope:]
        q_s[:, nope:] = (rope * cos_ref[...] + swap_halves(rope) * sin_ref[...]).astype(BF16)
        cols = slice(hh * nope, (hh + 1) * nope)
        w_kv = jnp.concatenate([wuk_ref[:, cols], wuv_ref[:, cols]], axis=1)
        kv = mm(lat_ref[...], w_kv).astype(BF16)
        k_s[:, :nope] = kv[:, :nope]
        k_s[:, nope:] = kr_ref[...]
        v_s[...] = kv[:, nope:]
        kt_s[...] = k_s[...].T
        vt_s[...] = v_s[...].T
        for i in range(n_blk):
            kl = (i + 1) * QBLK
            blk = slice(i * QBLK, kl)
            q_blk = q_s[blk, :]
            st = mm(k_s[:kl, :], q_blk, NT) * scale
            diag = jnp.where(causal, st[i * QBLK:, :], MASKED)
            st = diag if i == 0 else jnp.concatenate([st[:i * QBLK, :], diag], axis=0)
            top = jnp.max(st, axis=0, keepdims=True)
            pt = jnp.exp(st - top)
            pt = pt * (1.0 / jnp.sum(pt, axis=0, keepdims=True))
            pt_b = pt.astype(BF16)
            ot = mm(vt_s[:, :kl], pt_b)
            ot_st[slot, hh * nope:(hh + 1) * nope, blk] = ot.astype(BF16)
            dot_blk = dot_s[cols, blk]
            row_dot = jnp.sum(dot_blk.astype(F32) * ot, axis=0, keepdims=True)
            dpt = mm(v_s[:kl, :], dot_blk)
            dst = (pt * (dpt - row_dot) * scale).astype(BF16)
            dv_add = mm(pt_b, do_s[blk, cols])
            dk_add = mm(dst, q_blk)
            if i == 0:
                dv_acc[:kl, :] = dv_add
                dk_acc[:kl, :] = dk_add
            else:
                lo = i * QBLK
                dv_acc[:lo, :] += dv_add[:lo, :]
                dk_acc[:lo, :] += dk_add[:lo, :]
                dv_acc[lo:kl, :] = dv_add[lo:, :]
                dk_acc[lo:kl, :] = dk_add[lo:, :]
            dqt = mm(kt_s[:, :kl], dst)
            r1 = dqt[nope:nope + 32, :]
            r2 = dqt[nope + 32:nope + 64, :]
            c_t = cost_ref[:, blk]
            s_t = sint_ref[:, blk]
            dq_rot = jnp.concatenate([dqt[:nope, :], r1 * c_t + r2 * s_t, r2 * c_t - r1 * s_t], axis=0)
            dqt_st[slot, hh * qk:(hh + 1) * qk, blk] = dq_rot.astype(BF16)
        dk_st[slot, :, cols] = dk_acc[:, :nope].astype(BF16)
        dv_st[slot, :, cols] = dv_acc[...].astype(BF16)
        dkr_acc[...] += dk_acc[:, nope:]

    local, remote = copies(g, slot)
    for copy in local + remote:
        copy.start()

    @pl.when(g == n_pairs - 1)
    def _():
        kr_local = pltpu.make_async_copy(dkr_acc, dkr_out.at[core], kr_sem.at[0])
        kr_remote = pltpu.make_async_remote_copy(src_ref=dkr_acc, dst_ref=dkr_out.at[core], send_sem=kr_sem.at[1], recv_sem=kr_sem.at[2], device_id={'cp': partner}, device_id_type=pl.DeviceIdType.MESH)
        kr_local.start()
        kr_remote.start()
        for step in (n_pairs - 2, n_pairs - 1):
            local, remote = copies(step, step % 2)
            for copy in local:
                copy.wait()
            for copy in remote:
                copy.wait_send()
        for step in range(n_pairs):
            for copy in copies(step, step % 2)[1]:
                copy.wait_recv()
        kr_local.wait()
        kr_remote.wait()


def attention(x_all, gy_all, latent, kr_pad, cos_p, sin_p, cos_t, sin_t, wq_rows, wuk_cols, wuv_cols, wo_rows, scale):
    seq, width = x_all.shape
    nope = 128
    n_feat = wq_rows.shape[0]
    n_hv = wo_rows.shape[0]
    heads = n_hv // nope
    qk = n_feat // heads
    n_pairs = heads // 4
    const = lambda shape: pl.BlockSpec(shape, lambda g: (0, 0), pipeline_mode=pl.Buffered(1))
    mine = lambda g: lax.rem(lax.axis_index('cp'), 2) * n_pairs + g
    hbm = pl.BlockSpec(memory_space=pl.ANY)
    dma = pltpu.SemaphoreType.DMA
    vm = pltpu.VMEM
    return pl.pallas_call(
        functools.partial(attention_kernel, scale),
        grid=(n_pairs,),
        out_shape=(jax.ShapeDtypeStruct((n_hv, seq), BF16), jax.ShapeDtypeStruct((n_feat, seq), BF16), jax.ShapeDtypeStruct((seq, n_hv), BF16), jax.ShapeDtypeStruct((seq, n_hv), BF16), jax.ShapeDtypeStruct((2, seq, nope), F32)),
        in_specs=[const((seq, width)), const((seq, width)), const(latent.shape), const(kr_pad.shape), const(cos_p.shape), const(sin_p.shape), const(cos_t.shape), const(sin_t.shape),
                  pl.BlockSpec((2 * qk, width), lambda g: (mine(g), 0)), pl.BlockSpec((wuk_cols.shape[0], 2 * nope), lambda g: (0, mine(g))), pl.BlockSpec((wuv_cols.shape[0], 2 * nope), lambda g: (0, mine(g))), pl.BlockSpec((2 * nope, width), lambda g: (mine(g), 0))],
        out_specs=[hbm] * 5,
        scratch_shapes=[vm((seq, 256), BF16), vm((seq, 256), BF16), vm((256, seq), BF16), vm((seq, nope), BF16), vm((nope, seq), BF16), vm((seq, 2 * nope), BF16), vm((2 * nope, seq), BF16),
                        vm((seq, 256), F32), vm((seq, nope), F32), vm((seq, nope), F32),
                        vm((2, 2 * nope, seq), BF16), vm((2, 2 * qk, seq), BF16), vm((2, seq, 2 * nope), BF16), vm((2, seq, 2 * nope), BF16),
                        dma((2, 4)), dma((2, 4)), dma((n_pairs, 4)), dma((3,))],
        compiler_params=pltpu.CompilerParams(collective_id=1, has_side_effects=True, dimension_semantics=('arbitrary',), vmem_limit_bytes=60 * 1024 * 1024),
        name='attention_pairs',
    )(x_all, gy_all, latent, kr_pad, cos_p, sin_p, cos_t, sin_t, wq_rows, wuk_cols, wuv_cols, wo_rows)


def solution(mesh):
    n_dev = mesh.shape['cp']
    row_spec = P(('dp', 'cp'), None)
    in_specs = (row_spec, row_spec, P(), P(), P(), P(), P(), P(), P())
    out_specs = (row_spec, row_spec, P('dp', None, None), P('dp', None), P('dp'), P('dp', None), P('dp', None, None), P('dp', None, None), P('dp', None, None))

    def device_fn(x_loc, gy_loc, w_q, w_dkv, g_kv, w_kr, w_uk, w_uv, w_o):
        rows, width = x_loc.shape
        seq = rows * n_dev
        heads, qk = w_q.shape[1:]
        rope_dim = w_kr.shape[1]
        rank = w_dkv.shape[1]
        nope = qk - rope_dim
        scale = qk ** -0.5
        me = lax.axis_index('cp')
        half = rope_dim // 2
        inv_freq = ROPE_THETA ** (-(jnp.arange(half, dtype=F32) * 2.0 / rope_dim))
        angles = jnp.arange(seq, dtype=F32)[:, None] * inv_freq[None, :]
        cos, sin = jnp.cos(angles), jnp.sin(angles)
        zeros = jnp.zeros((seq, nope - rope_dim), F32)
        cos_p = jnp.concatenate([cos, cos, zeros], axis=1)
        sin_p = jnp.concatenate([-sin, sin, zeros], axis=1)
        cos_t, sin_t = cos.T, sin.T

        wq_rows = jnp.transpose(w_q, (1, 2, 0)).reshape(heads * qk, width)
        wo_rows = w_o.reshape(heads * nope, width)
        wuk_cols = w_uk.reshape(rank, heads * nope)
        wuv_cols = w_uv.reshape(rank, heads * nope)

        x_all, gy_all = gather_rows(x_loc, gy_loc, n_dev)

        c_raw = jnp.dot(x_all, w_dkv, preferred_element_type=F32)
        inv_rms = lax.rsqrt(jnp.mean(c_raw * c_raw, axis=-1, keepdims=True) + NORM_EPS)
        c_norm = c_raw * inv_rms
        g_f32 = g_kv.astype(F32)
        latent = (c_norm * g_f32).astype(BF16)
        kr_raw = jnp.dot(x_all, w_kr, preferred_element_type=F32)
        k1, k2 = kr_raw[:, :half], kr_raw[:, half:]
        kr_pad = jnp.concatenate([k1 * cos - k2 * sin, k2 * cos + k1 * sin, zeros], axis=1).astype(BF16)

        o_t, dq_t, dk, dv, dkr = attention(x_all, gy_all, latent, kr_pad, cos_p, sin_p, cos_t, sin_t, wq_rows, wuk_cols, wuv_cols, wo_rows, scale)

        own = lambda t: lax.dynamic_slice_in_dim(t, me * rows, rows, 0)
        own_t = lambda t: lax.dynamic_slice_in_dim(t, me * rows, rows, 1)
        tn = lambda a, b: lax.dot_general(a, b, (((0,), (0,)), ((), ())), preferred_element_type=F32)
        y_loc = tn(own_t(o_t), wo_rows).astype(BF16)
        gw_o = jnp.dot(o_t, gy_all, preferred_element_type=F32).reshape(w_o.shape)
        gw_q = jnp.transpose(jnp.dot(dq_t, x_all, preferred_element_type=F32).reshape(heads, qk, width), (2, 0, 1))
        gw_uk = tn(latent, dk).reshape(w_uk.shape)
        gw_uv = tn(latent, dv).reshape(w_uv.shape)
        d_latent = mm(dk, wuk_cols, NT) + mm(dv, wuv_cols, NT)
        gg_kv = jnp.sum(d_latent * c_norm, axis=0)
        d_norm = d_latent * g_f32
        dc_raw = (inv_rms * (d_norm - c_norm * jnp.mean(d_norm * c_norm, axis=-1, keepdims=True))).astype(BF16)
        d_kr = (dkr[0] + dkr[1])[:, :rope_dim]
        r1, r2 = d_kr[:, :half], d_kr[:, half:]
        dkr_raw = jnp.concatenate([r1 * cos + r2 * sin, r2 * cos - r1 * sin], axis=1).astype(BF16)
        gw_dkv = tn(x_all, dc_raw)
        gw_kr = tn(dkr_raw, x_all).T
        dx_loc = tn(own_t(dq_t), wq_rows) + mm(own(dc_raw), w_dkv, NT) + mm(own(dkr_raw), w_kr, NT)
        return (y_loc, dx_loc.astype(BF16), gw_q, gw_dkv, gg_kv, gw_kr, gw_uk, gw_uv, gw_o)

    return jax.shard_map(device_fn, mesh=mesh, in_specs=in_specs, out_specs=out_specs, check_vma=False)
```

```python
import functools

import jax
import jax.numpy as jnp
import numpy as np
from jax import lax
from jax.experimental import pallas as pl
from jax.experimental.pallas import tpu as pltpu
from jax.sharding import PartitionSpec as P

ROPE_THETA = 10000.0
NORM_EPS = 1e-6
QBLK = 256
MASKED = -1e30
LANES = 128
F32 = jnp.float32
BF16 = jnp.bfloat16
NN = (((1,), (0,)), ((), ()))
NT = (((1,), (1,)), ((), ()))
TN = (((0,), (0,)), ((), ()))


def mm(lhs, rhs, dims=NN):
    return lax.dot_general(lhs, rhs, dims, preferred_element_type=F32)


def swap_halves(t, half):
    return pltpu.roll(t, half, 1) + pltpu.roll(t, LANES - half, 1)


def block_kernel(n_chips, qk, scale, x_ref, gy_ref, tab_ref, wq_ref, wdkv_ref, gkv_ref, wkr_ref, wuk_ref, wuv_ref, wo_ref,
                 x_out, gy_out, lat_out, c_out, ot_out, dqt_out, dk_out, dv_out, dkr_out, y_out, dx_out,
                 x_s, gy_s, tab_s, tabt_s, wq_s, wdkv_s, wkr_s, wkv_raw, wkv_f32, wkv_s, wo_s, q_s, lat_s, c_s, kr_s, krt_s,
                 kn_s, v_s, kt_s, vt_s, lse_s, ot_st, do_s, dot_s, dk_acc, dv_acc, dkr_acc, y_acc, dx_acc, y_buf, dx_buf,
                 dqt_st, dk_st, dv_st,
                 ring_send, ring_recv, pr_send, pr_recv, w_sem, wq_sem, wo_sem, out_sem, loc_sem, snd_sem, rcv_sem, kr_sem, yx_sem):
    me = lax.axis_index('cp')
    core = lax.rem(me, 2)
    chip = lax.div(me, 2)
    partner = me + 1 - 2 * core
    ring_dev = (lax.rem(chip + 1, n_chips) * 2 + core, lax.rem(chip + n_chips - 1, n_chips) * 2 + core)
    rows = x_ref.shape[0]
    part = rows // 2
    both = 2 * rows
    seq = x_s.shape[0]
    heads = wq_s.shape[0]
    n_pairs = heads // 2
    nope = LANES
    rope_dim = wkr_ref.shape[0]
    half = rope_dim // 2
    far = n_chips // 2
    mesh_id = pl.DeviceIdType.MESH
    srcs, bufs = (x_ref, gy_ref), (x_s, gy_s)

    def origin(d, h):
        return lax.rem(chip + (n_chips - h if d == 0 else h), n_chips)

    def piece(arr, chip_of, core_of, p):
        start = pl.multiple_of((chip_of * 2 + core_of) * rows + p * part, part)
        return bufs[arr].at[pl.ds(start, part), :]

    def ring(arr, d, h, p, first=False):
        dst = piece(arr, origin(d, h), core, p)
        src = srcs[arr].at[pl.ds(p * part, part), :] if first else dst
        return pltpu.make_async_remote_copy(src_ref=src, dst_ref=dst, send_sem=ring_send.at[arr, d, h, p], recv_sem=ring_recv.at[arr, d, h, p], device_id={'cp': ring_dev[d]}, device_id_type=mesh_id)

    def across(arr, rel, p, first=False):
        dst = piece(arr, lax.rem(chip + n_chips - rel, n_chips), core, p)
        src = srcs[arr].at[pl.ds(p * part, part), :] if first else dst
        return pltpu.make_async_remote_copy(src_ref=src, dst_ref=dst, send_sem=pr_send.at[arr, rel, p], recv_sem=pr_recv.at[arr, rel, p], device_id={'cp': partner}, device_id_type=mesh_id)

    def hop(arr, h, p):
        for d in range(2):
            if isinstance(p, int):
                limit = far if d == p else far - 1
            else:
                limit = jnp.where(p == d, far, far - 1)

            @pl.when(h <= limit)
            def _():
                ring(arr, d, h - 1, p).wait_recv()

                @pl.when(h < limit)
                def _():
                    ring(arr, d, h, p).start()
                across(arr, h if d == 0 else n_chips - h, p).start()

    def weight_copies():
        first = core * heads
        out = [pltpu.make_async_copy(wdkv_ref, wdkv_s, w_sem.at[0]),
               pltpu.make_async_copy(wkr_ref, wkr_s.at[pl.ds(0, rope_dim), :], w_sem.at[1]),
               pltpu.make_async_copy(wuk_ref.at[:, pl.ds(pl.multiple_of(first, heads), heads), :], wkv_raw.at[0], w_sem.at[2]),
               pltpu.make_async_copy(wuv_ref.at[:, pl.ds(pl.multiple_of(first, heads), heads), :], wkv_raw.at[1], w_sem.at[3]),
               pltpu.make_async_copy(tab_ref, tab_s, w_sem.at[4])]
        for idx in range(2):
            out.append(pltpu.make_async_copy(srcs[idx], bufs[idx].at[pl.ds(pl.multiple_of(me * rows, rows), rows), :], w_sem.at[5 + idx]))
        for hh in range(heads):
            start = pl.multiple_of((first + hh) * qk, qk)
            out.append(pltpu.make_async_copy(wq_ref.at[pl.ds(start, qk), :], wq_s.at[hh, pl.ds(0, qk), :], wq_sem.at[hh]))
        return out

    def wo_copy(step):
        start = pl.multiple_of((core * n_pairs + step) * 2 * nope, 2 * nope)
        slot = lax.rem(step, 2)
        return pltpu.make_async_copy(wo_ref.at[pl.ds(start, 2 * nope), :], wo_s.at[slot], wo_sem.at[slot])

    barrier = pltpu.get_barrier_semaphore()
    for peer in (ring_dev[0], ring_dev[1], partner):
        pl.semaphore_signal(barrier, inc=1, device_id={'cp': peer}, device_id_type=mesh_id)
    for copy in weight_copies():
        copy.start()
    wo_copy(0).start()
    wo_copy(1).start()
    pl.semaphore_wait(barrier, 3)
    for p in range(2):
        for d in range(2):
            ring(0, d, 0, p, True).start()
    for arr in range(2):
        for p in range(2):
            across(arr, 0, p, True).start()

    wq_s[:, qk:, :] = jnp.zeros((heads, 2 * LANES - qk, wq_s.shape[2]), BF16)
    wkr_s[rope_dim:, :] = jnp.zeros((LANES - rope_dim, wkr_s.shape[1]), BF16)
    dkr_acc[...] = jnp.zeros_like(dkr_acc)
    y_acc[...] = jnp.zeros_like(y_acc)
    dx_acc[...] = jnp.zeros_like(dx_acc)
    for copy in weight_copies():
        copy.wait()
    tabt_s[...] = tab_s[...].T
    rank = wkv_raw.shape[1]
    for idx in range(2):
        wkv_f32[...] = wkv_raw[idx].astype(F32).reshape(rank * heads, LANES)
        for hh in range(heads):
            wkv_s[hh, :, idx * nope:(idx + 1) * nope] = wkv_f32[pl.ds(hh, rank, stride=heads), :].astype(BF16)

    lane = lax.broadcasted_iota(jnp.int32, (both, LANES), 1)

    def project(stage, starts):
        x_blk = jnp.concatenate([x_s[pl.ds(st, both), :] for st in starts], axis=0)
        cos_l, sin_l = [], []
        for st in starts:
            tab = tab_s[pl.ds(st, both), :]
            cos_l.append(jnp.where(lane < rope_dim, tab, 0.0))
            sin_l.append(jnp.where(lane < rope_dim, pltpu.roll(tab, rope_dim, 1), 0.0))
        cos_v, sin_v = jnp.concatenate(cos_l, axis=0), jnp.concatenate(sin_l, axis=0)

        def rotate(t):
            return (t * cos_v + swap_halves(t, half) * sin_v).astype(BF16)

        def put(ref, val):
            for idx, st in enumerate(starts):
                ref[pl.ds(st, both), :] = val[idx * both:(idx + 1) * both, :]

        if stage == 0:
            c_raw = mm(x_blk, wdkv_s[...])
            put(c_s, c_raw)
            inv_rms = lax.rsqrt(jnp.mean(c_raw * c_raw, axis=-1, keepdims=True) + NORM_EPS)
            put(lat_s, (c_raw * inv_rms * gkv_ref[...]).astype(BF16))
            put(kr_s, rotate(mm(x_blk, wkr_s[...], NT)))

        def head_pair(j, carry):
            for hh in range(2):
                h = stage * (heads // 2) + 2 * j + hh
                q_raw = mm(x_blk, wq_s[h], NT)
                q_val = jnp.concatenate([q_raw[:, :nope].astype(BF16), rotate(q_raw[:, nope:])], axis=1)
                for idx, st in enumerate(starts):
                    q_s[h, pl.ds(st, both), :] = q_val[idx * both:(idx + 1) * both, :]
            return carry
        lax.fori_loop(0, heads // 4, head_pair, 0)

    hop(0, 1, 0)
    hop(0, 1, 1)

    def x_stage(h, carry):
        near = h - 1
        up_rel = near
        dn_rel = jnp.where(near < far, n_chips - near, 0)
        chips = (lax.rem(chip + n_chips - up_rel, n_chips), lax.rem(chip + n_chips - dn_rel, n_chips))
        starts = [pl.multiple_of(c * both, both) for c in chips]

        @pl.when(h <= far)
        def _():
            hop(0, h, 0)

        @pl.when(h > far)
        def _():
            hop(1, 1, 0)
        for p in range(2):
            across(0, up_rel, p).wait_recv()
            across(0, dn_rel, p).wait_recv()
        project(0, starts)

        @pl.when(h <= far)
        def _():
            hop(0, h, 1)

        @pl.when(h == far - 1)
        def _():
            for p in range(2):
                for d in range(2):
                    ring(1, d, 0, p, True).start()

        @pl.when(h > far)
        def _():
            hop(1, 1, 1)
        project(1, starts)
        return carry
    lax.fori_loop(2, far + 2, x_stage, 0)

    outs = [pltpu.make_async_copy(src, dst, out_sem.at[idx]) for idx, (src, dst) in enumerate(((x_s, x_out), (lat_s, lat_out), (c_s, c_out), (gy_s, gy_out)))]
    for copy in outs[:3]:
        copy.start()
    krt_s[...] = kr_s[...].T

    row_id = lax.broadcasted_iota(jnp.int32, (QBLK, QBLK), 0)
    col_id = lax.broadcasted_iota(jnp.int32, (QBLK, QBLK), 1)
    causal = row_id <= col_id
    n_blk = seq // QBLK

    def scores(h, i):
        kl = (i + 1) * QBLK
        k_blk = jnp.concatenate([kn_s[h, :kl, :], kr_s[:kl, :]], axis=1)
        st = mm(k_blk, q_s[h, i * QBLK:kl, :], NT) * scale
        diag = jnp.where(causal, st[i * QBLK:, :], MASKED)
        return diag if i == 0 else jnp.concatenate([st[:i * QBLK, :], diag], axis=0)

    def forward(h, carry):
        @pl.when(h < 2 * (far - 1))
        def _():
            hop(1, 2 + lax.div(h, 2), lax.rem(h, 2))
        kv = mm(lat_s[...], wkv_s[h]).astype(BF16)
        kn_s[h] = kv[:, :nope]
        v_s[h] = kv[:, nope:]
        kt_s[h] = kv[:, :nope].T
        vt_s[...] = kv[:, nope:].T
        for i in range(n_blk):
            kl = (i + 1) * QBLK
            st = scores(h, i)
            top = jnp.max(st, axis=0, keepdims=True)
            pt = jnp.exp(st - top)
            total = jnp.sum(pt, axis=0, keepdims=True)
            ot = mm(vt_s[:, :kl], pt.astype(BF16)) * (1.0 / total)
            ot_st[pl.ds(pl.multiple_of(h * nope, nope), nope), i * QBLK:kl] = ot.astype(BF16)
            lse_s[h, :, i * QBLK:kl] = top + jnp.log(total)
        return carry
    lax.fori_loop(0, heads, forward, 0)

    ot_dst = ot_out.at[pl.ds(pl.multiple_of(core * heads * nope, heads * nope), heads * nope), :]
    ot_local = pltpu.make_async_copy(ot_st, ot_dst, kr_sem.at[3])
    ot_remote = pltpu.make_async_remote_copy(src_ref=ot_st, dst_ref=ot_dst, send_sem=kr_sem.at[4], recv_sem=kr_sem.at[5], device_id={'cp': partner}, device_id_type=mesh_id)
    ot_local.start()
    ot_remote.start()
    for rel in range(n_chips):
        for p in range(2):
            across(1, rel, p).wait_recv()
    outs[3].start()

    def pair_copies(step):
        slot_of = lax.rem(step, 2)
        pair = core * n_pairs + step
        col = pl.ds(pl.multiple_of(pair * 2 * nope, 2 * nope), 2 * nope)
        regions = ((dqt_st.at[slot_of], dqt_out.at[pl.ds(pl.multiple_of(pair * 2 * qk, 2 * qk), 2 * qk), :]), (dk_st.at[slot_of], dk_out.at[:, col]), (dv_st.at[slot_of], dv_out.at[:, col]))
        local, remote = [], []
        for idx, (src, dst) in enumerate(regions):
            local.append(pltpu.make_async_copy(src, dst, loc_sem.at[slot_of, idx]))
            remote.append(pltpu.make_async_remote_copy(src_ref=src, dst_ref=dst, send_sem=snd_sem.at[slot_of, idx], recv_sem=rcv_sem.at[step, idx], device_id={'cp': partner}, device_id_type=mesh_id))
        return local, remote

    chip_cols = pl.ds(pl.multiple_of(chip * both, both), both)

    def backward(g, carry):
        slot = lax.rem(g, 2)

        @pl.when(g >= 2)
        def _():
            local, remote = pair_copies(g - 2)
            for copy in local:
                copy.wait()
            for copy in remote:
                copy.wait_send()
        wo_copy(g).wait()
        do_all = mm(gy_s[...], wo_s[slot], NT).astype(BF16)
        do_s[...] = do_all
        dot_s[...] = do_all.T
        for hh in range(2):
            h = 2 * g + hh
            cols = slice(hh * nope, (hh + 1) * nope)
            for i in range(n_blk):
                kl = (i + 1) * QBLK
                lo = i * QBLK
                blk = slice(lo, kl)
                pt = jnp.exp(scores(h, i) - lse_s[h, :, blk])
                dpt = mm(v_s[h, :kl, :], dot_s[cols, blk])
                pdp = pt * dpt
                row_dot = jnp.sum(pdp, axis=0, keepdims=True)
                dst = ((pdp - pt * row_dot) * scale).astype(BF16)
                dv_add = mm(pt.astype(BF16), do_s[blk, cols])
                dk_add = mm(dst, q_s[h, blk, :])
                if i:
                    dv_acc[:lo, :] += dv_add[:lo, :]
                    dk_acc[:lo, :] += dk_add[:lo, :]
                dv_acc[blk, :] = dv_add[lo:, :]
                dk_acc[blk, :] = dk_add[lo:, :]
                kt_blk = jnp.concatenate([kt_s[h, :, :kl], krt_s[:, :kl]], axis=0)
                dqt = mm(kt_blk, dst)
                r1 = dqt[nope:nope + half, :]
                r2 = dqt[nope + half:nope + rope_dim, :]
                c_t = tabt_s[:half, blk]
                s_t = tabt_s[LANES - half:, blk]
                dqt_rot = jnp.concatenate([dqt[:nope, :], r1 * c_t + r2 * s_t, r2 * c_t - r1 * s_t], axis=0)
                dqt_st[slot, hh * qk:(hh + 1) * qk, blk] = dqt_rot.astype(BF16)
            dk_st[slot, :, cols] = dk_acc[:, :nope].astype(BF16)
            dv_st[slot, :, cols] = dv_acc[...].astype(BF16)
            dkr_acc[...] += dk_acc[:, nope:]
            dx_acc[...] += mm(dqt_st[slot, hh * qk:(hh + 1) * qk, chip_cols], wq_s[h, :qk, :], TN)
        local, remote = pair_copies(g)
        for copy in local + remote:
            copy.start()
        y_acc[...] += mm(ot_st[pl.ds(pl.multiple_of(g * 2 * nope, 2 * nope), 2 * nope), chip_cols], wo_s[slot], TN)

        @pl.when(g + 2 < n_pairs)
        def _():
            wo_copy(g + 2).start()
        return carry
    lax.fori_loop(0, n_pairs, backward, 0)

    theirs = pl.ds(pl.multiple_of((1 - core) * rows, rows), rows)
    mine = pl.ds(pl.multiple_of(core * rows, rows), rows)
    sums = [pltpu.make_async_remote_copy(src_ref=acc.at[theirs, :], dst_ref=buf, send_sem=yx_sem.at[idx], recv_sem=yx_sem.at[2 + idx], device_id={'cp': partner}, device_id_type=mesh_id) for idx, (acc, buf) in enumerate(((y_acc, y_buf), (dx_acc, dx_buf)))]
    kr_local = pltpu.make_async_copy(dkr_acc, dkr_out.at[core], kr_sem.at[0])
    kr_remote = pltpu.make_async_remote_copy(src_ref=dkr_acc, dst_ref=dkr_out.at[core], send_sem=kr_sem.at[1], recv_sem=kr_sem.at[2], device_id={'cp': partner}, device_id_type=mesh_id)
    for copy in sums + [kr_local, kr_remote]:
        copy.start()
    for arr in range(2):
        for p in range(2):
            for d in range(2):
                for h in range(far if d == p else far - 1):
                    ring(arr, d, h, p, h == 0).wait_send()
            for rel in range(n_chips):
                across(arr, rel, p, rel == 0).wait_send()
    for copy in outs:
        copy.wait()
    ot_local.wait()
    ot_remote.wait()
    for step in range(n_pairs):
        local, remote = pair_copies(step)
        if step >= n_pairs - 2:
            for copy in local:
                copy.wait()
            for copy in remote:
                copy.wait_send()
        for copy in remote:
            copy.wait_recv()
    kr_local.wait()
    kr_remote.wait()
    for copy in sums:
        copy.wait()
    y_out[...] = (y_acc[mine, :] + y_buf[...]).astype(BF16)
    dx_out[...] = dx_acc[mine, :] + dx_buf[...]


def block(x_loc, gy_loc, tab, wq_rows, w_dkv, g_row, wkr_t, w_uk, w_uv, wo_rows, n_dev, qk, scale):
    rows, width = x_loc.shape
    seq = rows * n_dev
    n_chips = n_dev // 2
    rank = w_dkv.shape[1]
    nope = LANES
    n_hv = wo_rows.shape[0]
    n_feat = wq_rows.shape[0]
    heads = n_hv // nope // 2
    n_pairs = heads // 2
    far = n_chips // 2
    hbm = pl.BlockSpec(memory_space=pl.ANY)
    vmem = pl.BlockSpec(memory_space=pltpu.VMEM)
    dma = pltpu.SemaphoreType.DMA
    vm = pltpu.VMEM
    sds = jax.ShapeDtypeStruct
    scratch = [vm((seq, width), BF16), vm((seq, width), BF16), vm((seq, LANES), F32), vm((LANES, seq), F32), vm((heads, 2 * LANES, width), BF16), vm((width, rank), BF16), vm((LANES, width), BF16),
               vm((2, rank, heads, nope), BF16), vm((rank * heads, nope), F32), vm((heads, rank, 2 * nope), BF16), vm((2, 2 * nope, width), BF16),
               vm((heads, seq, 2 * LANES), BF16), vm((seq, rank), BF16), vm((seq, rank), F32), vm((seq, LANES), BF16), vm((LANES, seq), BF16),
               vm((heads, seq, nope), BF16), vm((heads, seq, nope), BF16), vm((heads, nope, seq), BF16), vm((nope, seq), BF16), vm((heads, 1, seq), F32), vm((heads * nope, seq), BF16),
               vm((seq, 2 * nope), BF16), vm((2 * nope, seq), BF16), vm((seq, 2 * LANES), F32), vm((seq, nope), F32), vm((seq, LANES), F32),
               vm((2 * rows, width), F32), vm((2 * rows, width), F32), vm((rows, width), F32), vm((rows, width), F32),
               vm((2, 2 * qk, seq), BF16), vm((2, seq, 2 * nope), BF16), vm((2, seq, 2 * nope), BF16),
               dma((2, 2, far, 2)), dma((2, 2, far, 2)), dma((2, n_chips, 2)), dma((2, n_chips, 2)), dma((7,)), dma((heads,)), dma((2,)), dma((4,)), dma((2, 3)), dma((2, 3)), dma((n_pairs, 3)), dma((6,)), dma((4,))]
    return pl.pallas_call(
        functools.partial(block_kernel, n_chips, qk, scale),
        out_shape=(sds((seq, width), BF16), sds((seq, width), BF16), sds((seq, rank), BF16), sds((seq, rank), F32), sds((n_hv, seq), BF16), sds((n_feat, seq), BF16), sds((seq, n_hv), BF16), sds((seq, n_hv), BF16), sds((2, seq, LANES), F32), sds((rows, width), BF16), sds((rows, width), F32)),
        in_specs=[hbm] * 5 + [vmem] + [hbm] * 4,
        out_specs=[hbm] * 9 + [vmem] * 2,
        scratch_shapes=scratch,
        compiler_params=pltpu.CompilerParams(collective_id=0, has_side_effects=True, vmem_limit_bytes=67043328),
        name='latent_block',
    )(x_loc, gy_loc, tab, wq_rows, w_dkv, g_row, wkr_t, w_uk, w_uv, wo_rows)


def solution(mesh):
    n_dev = mesh.shape['cp']
    row_spec = P(('dp', 'cp'), None)
    in_specs = (row_spec, row_spec, P(), P(), P(), P(), P(), P(), P())
    out_specs = (row_spec, row_spec, P('dp', None, None), P('dp', None), P('dp'), P('dp', None), P('dp', None, None), P('dp', None, None), P('dp', None, None))

    def device_fn(x_loc, gy_loc, w_q, w_dkv, g_kv, w_kr, w_uk, w_uv, w_o):
        rows, width = x_loc.shape
        seq = rows * n_dev
        heads, qk = w_q.shape[1:]
        rope_dim = w_kr.shape[1]
        rank = w_dkv.shape[1]
        nope = qk - rope_dim
        scale = qk ** -0.5
        me = lax.axis_index('cp')
        half = rope_dim // 2
        inv_freq = ROPE_THETA ** (-(np.arange(half) * 2.0 / rope_dim))
        angles = np.arange(seq)[:, None] * inv_freq[None, :]
        cos, sin = np.cos(angles).astype(np.float32), np.sin(angles).astype(np.float32)
        tab = jnp.asarray(np.concatenate([cos, cos, -sin, sin], axis=1))

        wq_rows = jnp.transpose(w_q, (1, 2, 0)).reshape(heads * qk, width)
        wo_rows = w_o.reshape(heads * nope, width)
        wuk_cols = w_uk.reshape(rank, heads * nope)
        wuv_cols = w_uv.reshape(rank, heads * nope)
        g_f32 = g_kv.astype(F32)
        x_all, gy_all, latent, c_raw, o_t, dq_t, dk, dv, dkr, y_loc, dx_q = block(x_loc, gy_loc, tab, wq_rows, w_dkv, g_f32[None, :], w_kr.T, w_uk, w_uv, wo_rows, n_dev, qk, scale)
        inv_rms = lax.rsqrt(jnp.mean(c_raw * c_raw, axis=-1, keepdims=True) + NORM_EPS)
        c_norm = c_raw * inv_rms

        own = lambda t: lax.dynamic_slice_in_dim(t, me * rows, rows, 0)
        tn = lambda a, b: lax.dot_general(a, b, (((0,), (0,)), ((), ())), preferred_element_type=F32)
        gw_o = jnp.dot(o_t, gy_all, preferred_element_type=F32).reshape(w_o.shape)
        gw_q = jnp.transpose(jnp.dot(dq_t, x_all, preferred_element_type=F32).reshape(heads, qk, width), (2, 0, 1))
        gw_uk = tn(latent, dk).reshape(w_uk.shape)
        gw_uv = tn(latent, dv).reshape(w_uv.shape)
        d_latent = mm(dk, wuk_cols, NT) + mm(dv, wuv_cols, NT)
        gg_kv = jnp.sum(d_latent * c_norm, axis=0)
        d_norm = d_latent * g_f32
        dc_raw = (inv_rms * (d_norm - c_norm * jnp.mean(d_norm * c_norm, axis=-1, keepdims=True))).astype(BF16)
        d_kr = (dkr[0] + dkr[1])[:, :rope_dim]
        r1, r2 = d_kr[:, :half], d_kr[:, half:]
        cos, sin = tab[:, :half], tab[:, LANES - half:]
        dkr_raw = jnp.concatenate([r1 * cos + r2 * sin, r2 * cos - r1 * sin], axis=1).astype(BF16)
        gw_dkv = tn(x_all, dc_raw)
        gw_kr = tn(dkr_raw, x_all).T
        dx_loc = dx_q + mm(own(dc_raw), w_dkv, NT) + mm(own(dkr_raw), w_kr, NT)
        return (y_loc, dx_loc.astype(BF16), gw_q, gw_dkv, gg_kv, gw_kr, gw_uk, gw_uv, gw_o)

    return jax.shard_map(device_fn, mesh=mesh, in_specs=in_specs, out_specs=out_specs, check_vma=False)
```

```python
import functools

import jax
import jax.numpy as jnp
import numpy as np
from jax import lax
from jax.experimental import pallas as pl
from jax.experimental.pallas import tpu as pltpu
from jax.sharding import PartitionSpec as P

ROPE_THETA = 10000.0
NORM_EPS = 1e-6
QBLK = 256
MASKED = -1e30
LANES = 128
PARTS = 4
F32 = jnp.float32
BF16 = jnp.bfloat16
NN = (((1,), (0,)), ((), ()))
NT = (((1,), (1,)), ((), ()))
TN = (((0,), (0,)), ((), ()))


def mm(lhs, rhs, dims=NN):
    return lax.dot_general(lhs, rhs, dims, preferred_element_type=F32)


def swap_halves(t, half):
    return pltpu.roll(t, half, 1) + pltpu.roll(t, LANES - half, 1)


def block_kernel(n_chips, qk, scale, x_ref, gy_ref, tab_ref, wq_ref, wdkv_ref, gkv_ref, wkr_ref, wuk_ref, wuv_ref, wo_ref,
                 x_out, gy_out, lat_out, c_out, ot_out, dqt_out, dk_out, dv_out, dkr_out, y_out, dx_out,
                 x_s, gy_s, tab_s, tabt_s, wq_s, wdkv_s, wkr_s, wkv_raw, wkv_f32, wkv_s, wo_s, q_s, lat_s, c_s, kr_s, krt_s,
                 kn_s, v_s, kt_s, vt_s, lse_s, ot_st, do_s, dot_s, dk_acc, dv_acc, dkr_acc, y_acc, dx_acc, y_buf, dx_buf,
                 dqt_st, dk_st, dv_st,
                 ring_send, ring_recv, pr_send, pr_recv, w_sem, wq_sem, wo_sem, out_sem, loc_sem, snd_sem, rcv_sem, kr_sem, yx_sem):
    me = lax.axis_index('cp')
    core = lax.rem(me, 2)
    chip = lax.div(me, 2)
    partner = me + 1 - 2 * core
    ring_dev = (lax.rem(chip + 1, n_chips) * 2 + core, lax.rem(chip + n_chips - 1, n_chips) * 2 + core)
    rows = x_ref.shape[0]
    part = rows // PARTS
    both = 2 * rows
    seq = x_s.shape[0]
    heads = wq_s.shape[0]
    n_pairs = heads // 2
    nope = LANES
    rope_dim = wkr_ref.shape[0]
    half = rope_dim // 2
    far = n_chips // 2
    mesh_id = pl.DeviceIdType.MESH
    srcs, bufs = (x_ref, gy_ref), (x_s, gy_s)

    def origin(d, h):
        return lax.rem(chip + (n_chips - h if d == 0 else h), n_chips)

    def piece(arr, chip_of, core_of, p):
        start = pl.multiple_of((chip_of * 2 + core_of) * rows + p * part, part)
        return bufs[arr].at[pl.ds(start, part), :]

    def ring(arr, d, h, p, first=False):
        dst = piece(arr, origin(d, h), core, p)
        src = srcs[arr].at[pl.ds(p * part, part), :] if first else dst
        return pltpu.make_async_remote_copy(src_ref=src, dst_ref=dst, send_sem=ring_send.at[arr, d, h, p], recv_sem=ring_recv.at[arr, d, h, p], device_id={'cp': ring_dev[d]}, device_id_type=mesh_id)

    def across(arr, rel, p, first=False):
        dst = piece(arr, lax.rem(chip + n_chips - rel, n_chips), core, p)
        src = srcs[arr].at[pl.ds(p * part, part), :] if first else dst
        return pltpu.make_async_remote_copy(src_ref=src, dst_ref=dst, send_sem=pr_send.at[arr, rel, p], recv_sem=pr_recv.at[arr, rel, p], device_id={'cp': partner}, device_id_type=mesh_id)

    def hop(arr, h, p):
        for d in range(2):
            limit = jnp.where(lax.div(p, PARTS // 2) == d, far, far - 1)

            @pl.when(h <= limit)
            def _():
                ring(arr, d, h - 1, p).wait_recv()

                @pl.when(h < limit)
                def _():
                    ring(arr, d, h, p).start()
                across(arr, h if d == 0 else n_chips - h, p).start()

    def weight_copies():
        first = core * heads
        out = [pltpu.make_async_copy(wdkv_ref, wdkv_s, w_sem.at[0]),
               pltpu.make_async_copy(wkr_ref, wkr_s.at[pl.ds(0, rope_dim), :], w_sem.at[1]),
               pltpu.make_async_copy(wuk_ref.at[:, pl.ds(pl.multiple_of(first, heads), heads), :], wkv_raw.at[0], w_sem.at[2]),
               pltpu.make_async_copy(wuv_ref.at[:, pl.ds(pl.multiple_of(first, heads), heads), :], wkv_raw.at[1], w_sem.at[3]),
               pltpu.make_async_copy(tab_ref, tab_s, w_sem.at[4])]
        for idx in range(2):
            out.append(pltpu.make_async_copy(srcs[idx], bufs[idx].at[pl.ds(pl.multiple_of(me * rows, rows), rows), :], w_sem.at[5 + idx]))
        for hh in range(heads):
            start = pl.multiple_of((first + hh) * qk, qk)
            out.append(pltpu.make_async_copy(wq_ref.at[pl.ds(start, qk), :], wq_s.at[hh, pl.ds(0, qk), :], wq_sem.at[hh]))
        return out

    def wo_copy(step):
        start = pl.multiple_of((core * n_pairs + step) * 2 * nope, 2 * nope)
        slot = lax.rem(step, 2)
        return pltpu.make_async_copy(wo_ref.at[pl.ds(start, 2 * nope), :], wo_s.at[slot], wo_sem.at[slot])

    barrier = pltpu.get_barrier_semaphore()
    for peer in (ring_dev[0], ring_dev[1], partner):
        pl.semaphore_signal(barrier, inc=1, device_id={'cp': peer}, device_id_type=mesh_id)
    for copy in weight_copies():
        copy.start()
    wo_copy(0).start()
    wo_copy(1).start()
    pl.semaphore_wait(barrier, 3)
    for p in range(PARTS):
        for d in range(2):
            ring(0, d, 0, p, True).start()
    for arr in range(2):
        for p in range(PARTS):
            across(arr, 0, p, True).start()

    wq_s[:, qk:, :] = jnp.zeros((heads, 2 * LANES - qk, wq_s.shape[2]), BF16)
    wkr_s[rope_dim:, :] = jnp.zeros((LANES - rope_dim, wkr_s.shape[1]), BF16)
    dkr_acc[...] = jnp.zeros_like(dkr_acc)
    y_acc[...] = jnp.zeros_like(y_acc)
    dx_acc[...] = jnp.zeros_like(dx_acc)
    for copy in weight_copies():
        copy.wait()
    tabt_s[...] = tab_s[...].T
    rank = wkv_raw.shape[1]
    for idx in range(2):
        wkv_f32[...] = wkv_raw[idx].astype(F32).reshape(rank * heads, LANES)
        for hh in range(heads):
            wkv_s[hh, :, idx * nope:(idx + 1) * nope] = wkv_f32[pl.ds(hh, rank, stride=heads), :].astype(BF16)

    lane = lax.broadcasted_iota(jnp.int32, (2 * both, LANES), 1)

    def x_stage(h, carry):
        near = h - 1
        up_rel = near
        dn_rel = jnp.where(near < far, n_chips - near, 0)
        chips = (lax.rem(chip + n_chips - up_rel, n_chips), lax.rem(chip + n_chips - dn_rel, n_chips))
        starts = [pl.multiple_of(c * both, both) for c in chips]

        def rows_of(ref):
            return jnp.concatenate([ref[pl.ds(st, both), :] for st in starts], axis=0)

        def put(ref, val):
            for idx, st in enumerate(starts):
                ref[pl.ds(st, both), :] = val[idx * both:(idx + 1) * both, :]

        def rotate(t):
            tab = rows_of(tab_s)
            cos_v = jnp.where(lane < rope_dim, tab, 0.0)
            sin_v = jnp.where(lane < rope_dim, pltpu.roll(tab, rope_dim, 1), 0.0)
            return (t * cos_v + swap_halves(t, half) * sin_v).astype(BF16)

        def quarter(j, carry):
            @pl.when(h <= far)
            def _():
                hop(0, h, j)

            @pl.when(h > far)
            def _():
                hop(1, 1, j)

            @pl.when((h == far - 1) & (j == PARTS - 1))
            def _():
                for p in range(PARTS):
                    for d in range(2):
                        ring(1, d, 0, p, True).start()

            @pl.when(j == 0)
            def _():
                for p in range(PARTS):
                    across(0, up_rel, p).wait_recv()
                    across(0, dn_rel, p).wait_recv()
                x_blk = rows_of(x_s)
                c_raw = mm(x_blk, wdkv_s[...])
                put(c_s, c_raw)
                inv_rms = lax.rsqrt(jnp.mean(c_raw * c_raw, axis=-1, keepdims=True) + NORM_EPS)
                put(lat_s, (c_raw * inv_rms * gkv_ref[...]).astype(BF16))
                put(kr_s, rotate(mm(x_blk, wkr_s[...], NT)))
            x_blk = rows_of(x_s)
            for hh in range(heads // PARTS):
                head = j * (heads // PARTS) + hh
                q_raw = mm(x_blk, wq_s[head], NT)
                q_val = jnp.concatenate([q_raw[:, :nope].astype(BF16), rotate(q_raw[:, nope:])], axis=1)
                for idx, st in enumerate(starts):
                    q_s[head, pl.ds(st, both), :] = q_val[idx * both:(idx + 1) * both, :]
            return carry
        lax.fori_loop(0, PARTS, quarter, 0)
        return carry

    def first_hop(p, carry):
        hop(0, 1, p)
        return carry
    lax.fori_loop(0, PARTS, first_hop, 0)
    lax.fori_loop(2, far + 2, x_stage, 0)

    outs = [pltpu.make_async_copy(src, dst, out_sem.at[idx]) for idx, (src, dst) in enumerate(((x_s, x_out), (lat_s, lat_out), (c_s, c_out), (gy_s, gy_out)))]
    for copy in outs[:3]:
        copy.start()
    krt_s[...] = kr_s[...].T

    row_id = lax.broadcasted_iota(jnp.int32, (QBLK, QBLK), 0)
    col_id = lax.broadcasted_iota(jnp.int32, (QBLK, QBLK), 1)
    causal = row_id <= col_id
    n_blk = seq // QBLK

    def scores(h, i):
        kl = (i + 1) * QBLK
        k_blk = jnp.concatenate([kn_s[h, :kl, :], kr_s[:kl, :]], axis=1)
        st = mm(k_blk, q_s[h, i * QBLK:kl, :], NT) * scale
        diag = jnp.where(causal, st[i * QBLK:, :], MASKED)
        return diag if i == 0 else jnp.concatenate([st[:i * QBLK, :], diag], axis=0)

    def forward(h, carry):
        point = jnp.where(h < heads // 2, 2 * h, h + heads // 2)
        hop(1, 2 + lax.div(point, PARTS), lax.rem(point, PARTS))

        @pl.when(h < heads // 2)
        def _():
            hop(1, 2 + lax.div(point + 1, PARTS), lax.rem(point + 1, PARTS))
        kv = mm(lat_s[...], wkv_s[h]).astype(BF16)
        kn_s[h] = kv[:, :nope]
        v_s[h] = kv[:, nope:]
        kt_s[h] = kv[:, :nope].T
        vt_s[...] = kv[:, nope:].T
        for i in range(n_blk):
            kl = (i + 1) * QBLK
            st = scores(h, i)
            top = jnp.max(st, axis=0, keepdims=True)
            pt = jnp.exp(st - top)
            total = jnp.sum(pt, axis=0, keepdims=True)
            ot = mm(vt_s[:, :kl], pt.astype(BF16)) * (1.0 / total)
            ot_st[pl.ds(pl.multiple_of(h * nope, nope), nope), i * QBLK:kl] = ot.astype(BF16)
            lse_s[h, :, i * QBLK:kl] = top + jnp.log(total)
        return carry
    lax.fori_loop(0, heads, forward, 0)

    ot_dst = ot_out.at[pl.ds(pl.multiple_of(core * heads * nope, heads * nope), heads * nope), :]
    ot_local = pltpu.make_async_copy(ot_st, ot_dst, kr_sem.at[3])
    ot_remote = pltpu.make_async_remote_copy(src_ref=ot_st, dst_ref=ot_dst, send_sem=kr_sem.at[4], recv_sem=kr_sem.at[5], device_id={'cp': partner}, device_id_type=mesh_id)
    ot_local.start()
    ot_remote.start()
    for rel in range(n_chips):
        for p in range(PARTS):
            across(1, rel, p).wait_recv()
    outs[3].start()

    def pair_copies(step):
        slot_of = lax.rem(step, 2)
        pair = core * n_pairs + step
        col = pl.ds(pl.multiple_of(pair * 2 * nope, 2 * nope), 2 * nope)
        regions = ((dqt_st.at[slot_of], dqt_out.at[pl.ds(pl.multiple_of(pair * 2 * qk, 2 * qk), 2 * qk), :]), (dk_st.at[slot_of], dk_out.at[:, col]), (dv_st.at[slot_of], dv_out.at[:, col]))
        local, remote = [], []
        for idx, (src, dst) in enumerate(regions):
            local.append(pltpu.make_async_copy(src, dst, loc_sem.at[slot_of, idx]))
            remote.append(pltpu.make_async_remote_copy(src_ref=src, dst_ref=dst, send_sem=snd_sem.at[slot_of, idx], recv_sem=rcv_sem.at[step, idx], device_id={'cp': partner}, device_id_type=mesh_id))
        return local, remote

    chip_cols = pl.ds(pl.multiple_of(chip * both, both), both)

    def backward(g, carry):
        slot = lax.rem(g, 2)

        @pl.when(g >= 2)
        def _():
            local, remote = pair_copies(g - 2)
            for copy in local:
                copy.wait()
            for copy in remote:
                copy.wait_send()
        wo_copy(g).wait()
        do_all = mm(gy_s[...], wo_s[slot], NT).astype(BF16)
        do_s[...] = do_all
        dot_s[...] = do_all.T
        for hh in range(2):
            h = 2 * g + hh
            cols = slice(hh * nope, (hh + 1) * nope)
            for i in range(n_blk):
                kl = (i + 1) * QBLK
                lo = i * QBLK
                blk = slice(lo, kl)
                pt = jnp.exp(scores(h, i) - lse_s[h, :, blk])
                dpt = mm(v_s[h, :kl, :], dot_s[cols, blk])
                pdp = pt * dpt
                row_dot = jnp.sum(pdp, axis=0, keepdims=True)
                dst = ((pdp - pt * row_dot) * scale).astype(BF16)
                dv_add = mm(pt.astype(BF16), do_s[blk, cols])
                dk_add = mm(dst, q_s[h, blk, :])
                if i:
                    dv_acc[:lo, :] += dv_add[:lo, :]
                    dk_acc[:lo, :] += dk_add[:lo, :]
                dv_acc[blk, :] = dv_add[lo:, :]
                dk_acc[blk, :] = dk_add[lo:, :]
                kt_blk = jnp.concatenate([kt_s[h, :, :kl], krt_s[:, :kl]], axis=0)
                dqt = mm(kt_blk, dst)
                r1 = dqt[nope:nope + half, :]
                r2 = dqt[nope + half:nope + rope_dim, :]
                c_t = tabt_s[:half, blk]
                s_t = tabt_s[LANES - half:, blk]
                dqt_rot = jnp.concatenate([dqt[:nope, :], r1 * c_t + r2 * s_t, r2 * c_t - r1 * s_t], axis=0)
                dqt_st[slot, hh * qk:(hh + 1) * qk, blk] = dqt_rot.astype(BF16)
            dk_st[slot, :, cols] = dk_acc[:, :nope].astype(BF16)
            dv_st[slot, :, cols] = dv_acc[...].astype(BF16)
            dkr_acc[...] += dk_acc[:, nope:]
            dx_acc[...] += mm(dqt_st[slot, hh * qk:(hh + 1) * qk, chip_cols], wq_s[h, :qk, :], TN)
        local, remote = pair_copies(g)
        for copy in local + remote:
            copy.start()
        y_acc[...] += mm(ot_st[pl.ds(pl.multiple_of(g * 2 * nope, 2 * nope), 2 * nope), chip_cols], wo_s[slot], TN)

        @pl.when(g + 2 < n_pairs)
        def _():
            wo_copy(g + 2).start()
        return carry
    lax.fori_loop(0, n_pairs, backward, 0)

    theirs = pl.ds(pl.multiple_of((1 - core) * rows, rows), rows)
    mine = pl.ds(pl.multiple_of(core * rows, rows), rows)
    sums = [pltpu.make_async_remote_copy(src_ref=acc.at[theirs, :], dst_ref=buf, send_sem=yx_sem.at[idx], recv_sem=yx_sem.at[2 + idx], device_id={'cp': partner}, device_id_type=mesh_id) for idx, (acc, buf) in enumerate(((y_acc, y_buf), (dx_acc, dx_buf)))]
    kr_local = pltpu.make_async_copy(dkr_acc, dkr_out.at[core], kr_sem.at[0])
    kr_remote = pltpu.make_async_remote_copy(src_ref=dkr_acc, dst_ref=dkr_out.at[core], send_sem=kr_sem.at[1], recv_sem=kr_sem.at[2], device_id={'cp': partner}, device_id_type=mesh_id)
    for copy in sums + [kr_local, kr_remote]:
        copy.start()
    for arr in range(2):
        for p in range(PARTS):
            for d in range(2):
                for h in range(far if d == p // (PARTS // 2) else far - 1):
                    ring(arr, d, h, p, h == 0).wait_send()
            for rel in range(n_chips):
                across(arr, rel, p, rel == 0).wait_send()
    for copy in outs:
        copy.wait()
    ot_local.wait()
    ot_remote.wait()
    for step in range(n_pairs):
        local, remote = pair_copies(step)
        if step >= n_pairs - 2:
            for copy in local:
                copy.wait()
            for copy in remote:
                copy.wait_send()
        for copy in remote:
            copy.wait_recv()
    kr_local.wait()
    kr_remote.wait()
    for copy in sums:
        copy.wait()
    y_out[...] = (y_acc[mine, :] + y_buf[...]).astype(BF16)
    dx_out[...] = dx_acc[mine, :] + dx_buf[...]


def block(x_loc, gy_loc, tab, wq_rows, w_dkv, g_row, wkr_t, w_uk, w_uv, wo_rows, n_dev, qk, scale):
    rows, width = x_loc.shape
    seq = rows * n_dev
    n_chips = n_dev // 2
    rank = w_dkv.shape[1]
    nope = LANES
    n_hv = wo_rows.shape[0]
    n_feat = wq_rows.shape[0]
    heads = n_hv // nope // 2
    n_pairs = heads // 2
    far = n_chips // 2
    hbm = pl.BlockSpec(memory_space=pl.ANY)
    vmem = pl.BlockSpec(memory_space=pltpu.VMEM)
    dma = pltpu.SemaphoreType.DMA
    vm = pltpu.VMEM
    sds = jax.ShapeDtypeStruct
    scratch = [vm((seq, width), BF16), vm((seq, width), BF16), vm((seq, LANES), F32), vm((LANES, seq), F32), vm((heads, 2 * LANES, width), BF16), vm((width, rank), BF16), vm((LANES, width), BF16),
               vm((2, rank, heads, nope), BF16), vm((rank * heads, nope), F32), vm((heads, rank, 2 * nope), BF16), vm((2, 2 * nope, width), BF16),
               vm((heads, seq, 2 * LANES), BF16), vm((seq, rank), BF16), vm((seq, rank), F32), vm((seq, LANES), BF16), vm((LANES, seq), BF16),
               vm((heads, seq, nope), BF16), vm((heads, seq, nope), BF16), vm((heads, nope, seq), BF16), vm((nope, seq), BF16), vm((heads, 1, seq), F32), vm((heads * nope, seq), BF16),
               vm((seq, 2 * nope), BF16), vm((2 * nope, seq), BF16), vm((seq, 2 * LANES), F32), vm((seq, nope), F32), vm((seq, LANES), F32),
               vm((2 * rows, width), F32), vm((2 * rows, width), F32), vm((rows, width), F32), vm((rows, width), F32),
               vm((2, 2 * qk, seq), BF16), vm((2, seq, 2 * nope), BF16), vm((2, seq, 2 * nope), BF16),
               dma((2, 2, far, PARTS)), dma((2, 2, far, PARTS)), dma((2, n_chips, PARTS)), dma((2, n_chips, PARTS)), dma((7,)), dma((heads,)), dma((2,)), dma((4,)), dma((2, 3)), dma((2, 3)), dma((n_pairs, 3)), dma((6,)), dma((4,))]
    return pl.pallas_call(
        functools.partial(block_kernel, n_chips, qk, scale),
        out_shape=(sds((seq, width), BF16), sds((seq, width), BF16), sds((seq, rank), BF16), sds((seq, rank), F32), sds((n_hv, seq), BF16), sds((n_feat, seq), BF16), sds((seq, n_hv), BF16), sds((seq, n_hv), BF16), sds((2, seq, LANES), F32), sds((rows, width), BF16), sds((rows, width), F32)),
        in_specs=[hbm] * 5 + [vmem] + [hbm] * 4,
        out_specs=[hbm] * 9 + [vmem] * 2,
        scratch_shapes=scratch,
        compiler_params=pltpu.CompilerParams(collective_id=0, has_side_effects=True, vmem_limit_bytes=67043328),
        name='latent_block',
    )(x_loc, gy_loc, tab, wq_rows, w_dkv, g_row, wkr_t, w_uk, w_uv, wo_rows)


def grads_kernel(tile, ot_ref, dqt_ref, gy_ref, x_ref, lat_ref, dk_ref, dv_ref, gwo_ref, gwq_ref, guk_ref, guv_ref,
                 lhs_s, rhs_s, lat_s, latt_s, kv_s, stage, stage_kv, in_sem, out_sem, kv_sem):
    n_o, n_q = ot_ref.shape[0] // tile, dqt_ref.shape[0] // tile
    heads = kv_s.shape[2] // LANES
    rank = lat_s.shape[1]
    n_c = rank // tile
    rest = [(ot_ref.at[pl.ds(tile, (n_o - 1) * tile), :], lhs_s.at[pl.ds(tile, (n_o - 1) * tile), :]), (x_ref, rhs_s.at[1]), (dqt_ref, lhs_s.at[pl.ds(n_o * tile, n_q * tile), :]), (lat_ref, lat_s), (dk_ref, kv_s.at[0]), (dv_ref, kv_s.at[1])]
    loads = [pltpu.make_async_copy(src, dst, in_sem.at[idx]) for idx, (src, dst) in enumerate([(ot_ref.at[pl.ds(0, tile), :], lhs_s.at[pl.ds(0, tile), :]), (gy_ref, rhs_s.at[0])] + rest)]
    for copy in loads:
        copy.start()

    def out_copy(t, dst, base):
        slot = lax.rem(t, 2)
        return pltpu.make_async_copy(stage.at[slot], dst.at[pl.ds(pl.multiple_of((t - base) * tile, tile), tile), :], out_sem.at[slot])

    loads[0].wait()
    loads[1].wait()

    def product(t, carry):
        slot = lax.rem(t, 2)

        @pl.when(t == 1)
        def _():
            loads[2].wait()

        @pl.when(t == n_o)
        def _():
            loads[3].wait()
            loads[4].wait()

        @pl.when(t >= 2)
        def _():
            out_copy(t, gwo_ref, t).wait()
        which = jnp.where(t < n_o, 0, 1)
        stage[slot] = mm(lhs_s[pl.ds(pl.multiple_of(t * tile, tile), tile), :], rhs_s[which])

        @pl.when(t < n_o)
        def _():
            out_copy(t, gwo_ref, 0).start()

        @pl.when(t >= n_o)
        def _():
            out_copy(t, gwq_ref, n_o).start()
        return carry
    lax.fori_loop(0, n_o + n_q, product, 0)
    for copy in loads[5:]:
        copy.wait()
    latt_s[...] = lat_s[...].T

    def kv_copy(t, dst, base):
        slot = lax.rem(t, 2)
        size = tile * heads
        return pltpu.make_async_copy(stage_kv.at[slot], dst.at[pl.ds(pl.multiple_of((t - base) * size, size), size), :], kv_sem.at[slot])

    def latent_side(t, carry):
        slot = lax.rem(t, 2)

        @pl.when(t >= 2)
        def _():
            kv_copy(t, guk_ref, t).wait()
        which = jnp.where(t < n_c, 0, 1)
        row = pl.multiple_of((t - which * n_c) * tile, tile)
        res = mm(latt_s[pl.ds(row, tile), :], kv_s[which])
        for h in range(heads):
            stage_kv[slot, pl.ds(h, tile, stride=heads), :] = res[:, h * LANES:(h + 1) * LANES]

        @pl.when(t < n_c)
        def _():
            kv_copy(t, guk_ref, 0).start()

        @pl.when(t >= n_c)
        def _():
            kv_copy(t, guv_ref, n_c).start()
        return carry
    lax.fori_loop(0, 2 * n_c, latent_side, 0)
    for t in range(2):
        out_copy(t, gwo_ref, t).wait()
        kv_copy(t, guk_ref, t).wait()


def big_grads(o_t, dq_t, gy_all, x_all, latent, dk, dv):
    tile = 256
    seq, width = x_all.shape
    n_hv, n_feat, rank = o_t.shape[0], dq_t.shape[0], latent.shape[1]
    heads = n_hv // LANES
    hbm = pl.BlockSpec(memory_space=pl.ANY)
    dma = pltpu.SemaphoreType.DMA
    vm = pltpu.VMEM
    sds = jax.ShapeDtypeStruct
    flops = 2 * seq * width * (n_hv + n_feat) + 4 * seq * rank * n_hv
    return pl.pallas_call(
        functools.partial(grads_kernel, tile),
        out_shape=(sds((n_hv, width), F32), sds((n_feat, width), F32), sds((rank * heads, LANES), F32), sds((rank * heads, LANES), F32)),
        in_specs=[hbm] * 7,
        out_specs=[hbm] * 4,
        scratch_shapes=[vm((n_hv + n_feat, seq), BF16), vm((2, seq, width), BF16), vm((seq, rank), BF16), vm((rank, seq), BF16), vm((2, seq, n_hv), BF16), vm((2, tile, width), F32), vm((2, tile * heads, LANES), F32), dma((8,)), dma((2,)), dma((2,))],
        compiler_params=pltpu.CompilerParams(vmem_limit_bytes=56 * 1024 * 1024),
        cost_estimate=pl.CostEstimate(flops=flops, bytes_accessed=80 * 1024 * 1024, transcendentals=0),
        name='weight_grads',
    )(o_t, dq_t, gy_all, x_all, latent, dk, dv)


def solution(mesh):
    n_dev = mesh.shape['cp']
    row_spec = P(('dp', 'cp'), None)
    in_specs = (row_spec, row_spec, P(), P(), P(), P(), P(), P(), P())
    out_specs = (row_spec, row_spec, P('dp', None, None), P('dp', None), P('dp'), P('dp', None), P('dp', None, None), P('dp', None, None), P('dp', None, None))

    def device_fn(x_loc, gy_loc, w_q, w_dkv, g_kv, w_kr, w_uk, w_uv, w_o):
        rows, width = x_loc.shape
        seq = rows * n_dev
        heads, qk = w_q.shape[1:]
        rope_dim = w_kr.shape[1]
        rank = w_dkv.shape[1]
        nope = qk - rope_dim
        scale = qk ** -0.5
        me = lax.axis_index('cp')
        half = rope_dim // 2
        inv_freq = ROPE_THETA ** (-(np.arange(half) * 2.0 / rope_dim))
        angles = np.arange(seq)[:, None] * inv_freq[None, :]
        cos, sin = np.cos(angles).astype(np.float32), np.sin(angles).astype(np.float32)
        tab = jnp.asarray(np.concatenate([cos, cos, -sin, sin], axis=1))

        wq_rows = jnp.transpose(w_q, (1, 2, 0)).reshape(heads * qk, width)
        wo_rows = w_o.reshape(heads * nope, width)
        wuk_cols = w_uk.reshape(rank, heads * nope)
        wuv_cols = w_uv.reshape(rank, heads * nope)
        g_f32 = g_kv.astype(F32)
        x_all, gy_all, latent, c_raw, o_t, dq_t, dk, dv, dkr, y_loc, dx_q = block(x_loc, gy_loc, tab, wq_rows, w_dkv, g_f32[None, :], w_kr.T, w_uk, w_uv, wo_rows, n_dev, qk, scale)
        inv_rms = lax.rsqrt(jnp.mean(c_raw * c_raw, axis=-1, keepdims=True) + NORM_EPS)
        c_norm = c_raw * inv_rms

        own = lambda t: lax.dynamic_slice_in_dim(t, me * rows, rows, 0)
        tn = lambda a, b: lax.dot_general(a, b, (((0,), (0,)), ((), ())), preferred_element_type=F32)
        gwo, gwq, guk, guv = big_grads(o_t, dq_t, gy_all, x_all, latent, dk, dv)
        gw_o = gwo.reshape(w_o.shape)
        gw_q = jnp.transpose(gwq.reshape(heads, qk, width), (2, 0, 1))
        gw_uk, gw_uv = guk.reshape(w_uk.shape), guv.reshape(w_uv.shape)
        d_latent = mm(dk, wuk_cols, NT) + mm(dv, wuv_cols, NT)
        gg_kv = jnp.sum(d_latent * c_norm, axis=0)
        d_norm = d_latent * g_f32
        dc_raw = (inv_rms * (d_norm - c_norm * jnp.mean(d_norm * c_norm, axis=-1, keepdims=True))).astype(BF16)
        d_kr = (dkr[0] + dkr[1])[:, :rope_dim]
        r1, r2 = d_kr[:, :half], d_kr[:, half:]
        cos, sin = tab[:, :half], tab[:, LANES - half:]
        dkr_raw = jnp.concatenate([r1 * cos + r2 * sin, r2 * cos - r1 * sin], axis=1).astype(BF16)
        gw_dkv = tn(x_all, dc_raw)
        gw_kr = tn(dkr_raw, x_all).T
        dx_loc = dx_q + mm(own(dc_raw), w_dkv, NT) + mm(own(dkr_raw), w_kr, NT)
        return (y_loc, dx_loc.astype(BF16), gw_q, gw_dkv, gg_kv, gw_kr, gw_uk, gw_uv, gw_o)

    return jax.shard_map(device_fn, mesh=mesh, in_specs=in_specs, out_specs=out_specs, check_vma=False)
```

```python
import functools

import jax
import jax.numpy as jnp
import numpy as np
from jax import lax
from jax.experimental import pallas as pl
from jax.experimental.pallas import tpu as pltpu
from jax.sharding import PartitionSpec as P

ROPE_THETA = 10000.0
NORM_EPS = 1e-6
QBLK = 256
MASKED = -1e30
LANES = 128
PARTS = 4
F32 = jnp.float32
BF16 = jnp.bfloat16
NN = (((1,), (0,)), ((), ()))
NT = (((1,), (1,)), ((), ()))
TN = (((0,), (0,)), ((), ()))


def mm(lhs, rhs, dims=NN):
    return lax.dot_general(lhs, rhs, dims, preferred_element_type=F32)


def swap_halves(t, half):
    return pltpu.roll(t, half, 1) + pltpu.roll(t, LANES - half, 1)


def block_kernel(n_chips, qk, scale, x_ref, gy_ref, tab_ref, wq_ref, wdkv_ref, gkv_ref, wkr_ref, wuk_ref, wuv_ref, wo_ref,
                 x_out, gy_out, lat_out, c_out, ot_out, dqt_out, dk_out, dv_out, dkr_out, dlat_out, y_out, dx_out,
                 x_s, gy_s, tab_s, tabt_s, wq_s, wdkv_s, wkr_s, wkv_raw, wkv_f32, wkv_s, wo_s, q_s, lat_s, c_s, kr_s, krt_s,
                 kn_s, v_s, kt_s, vt_s, lse_s, ot_st, do_s, dot_s, dk_acc, dv_acc, dkr_acc, y_acc, dx_acc, y_buf, dx_buf,
                 dqt_st, dk_st, dv_st,
                 ring_send, ring_recv, pr_send, pr_recv, w_sem, wq_sem, wo_sem, out_sem, loc_sem, snd_sem, rcv_sem, kr_sem, yx_sem, dlat_sem):
    me = lax.axis_index('cp')
    core = lax.rem(me, 2)
    chip = lax.div(me, 2)
    partner = me + 1 - 2 * core
    ring_dev = (lax.rem(chip + 1, n_chips) * 2 + core, lax.rem(chip + n_chips - 1, n_chips) * 2 + core)
    rows = x_ref.shape[0]
    part = rows // PARTS
    both = 2 * rows
    seq = x_s.shape[0]
    heads = wq_s.shape[0]
    n_pairs = heads // 2
    nope = LANES
    rope_dim = wkr_ref.shape[0]
    half = rope_dim // 2
    far = n_chips // 2
    mesh_id = pl.DeviceIdType.MESH
    srcs, bufs = (x_ref, gy_ref), (x_s, gy_s)

    def origin(d, h):
        return lax.rem(chip + (n_chips - h if d == 0 else h), n_chips)

    def piece(arr, chip_of, core_of, p):
        start = pl.multiple_of((chip_of * 2 + core_of) * rows + p * part, part)
        return bufs[arr].at[pl.ds(start, part), :]

    def ring(arr, d, h, p, first=False):
        dst = piece(arr, origin(d, h), core, p)
        src = srcs[arr].at[pl.ds(p * part, part), :] if first else dst
        return pltpu.make_async_remote_copy(src_ref=src, dst_ref=dst, send_sem=ring_send.at[arr, d, h, p], recv_sem=ring_recv.at[arr, d, h, p], device_id={'cp': ring_dev[d]}, device_id_type=mesh_id)

    def across(arr, rel, p, first=False):
        dst = piece(arr, lax.rem(chip + n_chips - rel, n_chips), core, p)
        src = srcs[arr].at[pl.ds(p * part, part), :] if first else dst
        return pltpu.make_async_remote_copy(src_ref=src, dst_ref=dst, send_sem=pr_send.at[arr, rel, p], recv_sem=pr_recv.at[arr, rel, p], device_id={'cp': partner}, device_id_type=mesh_id)

    def hop(arr, h, p):
        for d in range(2):
            limit = jnp.where(lax.div(p, PARTS // 2) == d, far, far - 1)

            @pl.when(h <= limit)
            def _():
                ring(arr, d, h - 1, p).wait_recv()

                @pl.when(h < limit)
                def _():
                    ring(arr, d, h, p).start()
                across(arr, h if d == 0 else n_chips - h, p).start()

    def weight_copies():
        first = core * heads
        out = [pltpu.make_async_copy(wuk_ref.at[:, pl.ds(pl.multiple_of(first, heads), heads), :], wkv_raw.at[0], w_sem.at[2]),
               pltpu.make_async_copy(wuv_ref.at[:, pl.ds(pl.multiple_of(first, heads), heads), :], wkv_raw.at[1], w_sem.at[3]),
               pltpu.make_async_copy(wkr_ref, wkr_s.at[pl.ds(0, rope_dim), :], w_sem.at[1]),
               pltpu.make_async_copy(tab_ref, tab_s, w_sem.at[4]),
               pltpu.make_async_copy(wdkv_ref, wdkv_s, w_sem.at[0])]
        for idx in range(2):
            out.append(pltpu.make_async_copy(srcs[idx], bufs[idx].at[pl.ds(pl.multiple_of(me * rows, rows), rows), :], w_sem.at[5 + idx]))
        for hh in range(heads):
            start = pl.multiple_of((first + hh) * qk, qk)
            out.append(pltpu.make_async_copy(wq_ref.at[pl.ds(start, qk), :], wq_s.at[hh, pl.ds(0, qk), :], wq_sem.at[hh]))
        return out

    def wo_copy(step):
        start = pl.multiple_of((core * n_pairs + step) * 2 * nope, 2 * nope)
        slot = lax.rem(step, 2)
        return pltpu.make_async_copy(wo_ref.at[pl.ds(start, 2 * nope), :], wo_s.at[slot], wo_sem.at[slot])

    barrier = pltpu.get_barrier_semaphore()
    for peer in (ring_dev[0], ring_dev[1], partner):
        pl.semaphore_signal(barrier, inc=1, device_id={'cp': peer}, device_id_type=mesh_id)
    pl.semaphore_wait(barrier, 3)
    for p in range(PARTS):
        for d in range(2):
            ring(0, d, 0, p, True).start()
    for arr in range(2):
        for p in range(PARTS):
            across(arr, 0, p, True).start()
    for copy in weight_copies():
        copy.start()
    wo_copy(0).start()
    wo_copy(1).start()

    weights = weight_copies()
    rank = wkv_raw.shape[1]
    for p in range(PARTS):
        hop(0, 1, p)
        if p == 0:
            wq_s[:, qk:, :] = jnp.zeros((heads, 2 * LANES - qk, wq_s.shape[2]), BF16)
            wkr_s[rope_dim:, :] = jnp.zeros((LANES - rope_dim, wkr_s.shape[1]), BF16)
            dkr_acc[...] = jnp.zeros_like(dkr_acc)
            y_acc[...] = jnp.zeros_like(y_acc)
            dx_acc[...] = jnp.zeros_like(dx_acc)
        elif p <= 2:
            idx = p - 1
            weights[idx].wait()
            wkv_f32[...] = wkv_raw[idx].astype(F32).reshape(rank * heads, LANES)
            for hh in range(heads):
                wkv_s[hh, :, idx * nope:(idx + 1) * nope] = wkv_f32[pl.ds(hh, rank, stride=heads), :].astype(BF16)
    for copy in weights[2:]:
        copy.wait()
    tabt_s[...] = tab_s[...].T

    lane = lax.broadcasted_iota(jnp.int32, (2 * both, LANES), 1)

    def x_stage(h, carry):
        near = h - 1
        up_rel = near
        dn_rel = jnp.where(near < far, n_chips - near, 0)
        chips = (lax.rem(chip + n_chips - up_rel, n_chips), lax.rem(chip + n_chips - dn_rel, n_chips))
        starts = [pl.multiple_of(c * both, both) for c in chips]

        def rows_of(ref):
            return jnp.concatenate([ref[pl.ds(st, both), :] for st in starts], axis=0)

        def put(ref, val):
            for idx, st in enumerate(starts):
                ref[pl.ds(st, both), :] = val[idx * both:(idx + 1) * both, :]

        def rotate(t):
            tab = rows_of(tab_s)
            cos_v = jnp.where(lane < rope_dim, tab, 0.0)
            sin_v = jnp.where(lane < rope_dim, pltpu.roll(tab, rope_dim, 1), 0.0)
            return (t * cos_v + swap_halves(t, half) * sin_v).astype(BF16)

        def quarter(j, carry):
            @pl.when(h <= far)
            def _():
                hop(0, h, j)

            @pl.when(h > far)
            def _():
                hop(1, 1, j)

            @pl.when((h == far - 1) & (j == PARTS - 1))
            def _():
                for p in range(PARTS):
                    for d in range(2):
                        ring(1, d, 0, p, True).start()

            @pl.when(j == 0)
            def _():
                for p in range(PARTS):
                    across(0, up_rel, p).wait_recv()
                    across(0, dn_rel, p).wait_recv()
                x_blk = rows_of(x_s)
                c_raw = mm(x_blk, wdkv_s[...])
                put(c_s, c_raw)
                inv_rms = lax.rsqrt(jnp.mean(c_raw * c_raw, axis=-1, keepdims=True) + NORM_EPS)
                put(lat_s, (c_raw * inv_rms * gkv_ref[...]).astype(BF16))
                put(kr_s, rotate(mm(x_blk, wkr_s[...], NT)))
            x_blk = rows_of(x_s)
            for hh in range(heads // PARTS):
                head = j * (heads // PARTS) + hh
                q_raw = mm(x_blk, wq_s[head], NT)
                q_val = jnp.concatenate([q_raw[:, :nope].astype(BF16), rotate(q_raw[:, nope:])], axis=1)
                for idx, st in enumerate(starts):
                    q_s[head, pl.ds(st, both), :] = q_val[idx * both:(idx + 1) * both, :]
            return carry
        lax.fori_loop(0, PARTS, quarter, 0)
        return carry

    lax.fori_loop(2, far + 2, x_stage, 0)

    outs = [pltpu.make_async_copy(src, dst, out_sem.at[idx]) for idx, (src, dst) in enumerate(((x_s, x_out), (lat_s, lat_out), (c_s, c_out), (gy_s, gy_out)))]
    for copy in outs[:3]:
        copy.start()
    krt_s[...] = kr_s[...].T

    row_id = lax.broadcasted_iota(jnp.int32, (QBLK, QBLK), 0)
    col_id = lax.broadcasted_iota(jnp.int32, (QBLK, QBLK), 1)
    causal = row_id <= col_id
    n_blk = seq // QBLK

    def scores(h, i):
        kl = (i + 1) * QBLK
        k_blk = jnp.concatenate([kn_s[h, :kl, :], kr_s[:kl, :]], axis=1)
        st = mm(k_blk, q_s[h, i * QBLK:kl, :], NT) * scale
        diag = jnp.where(causal, st[i * QBLK:, :], MASKED)
        return diag if i == 0 else jnp.concatenate([st[:i * QBLK, :], diag], axis=0)

    def forward(h, carry):
        point = jnp.where(h < heads // 2, 2 * h, h + heads // 2)
        hop(1, 2 + lax.div(point, PARTS), lax.rem(point, PARTS))

        @pl.when(h < heads // 2)
        def _():
            hop(1, 2 + lax.div(point + 1, PARTS), lax.rem(point + 1, PARTS))
        kv = mm(lat_s[...], wkv_s[h]).astype(BF16)
        kn_s[h] = kv[:, :nope]
        v_s[h] = kv[:, nope:]
        kt_s[h] = kv[:, :nope].T
        vt_s[...] = kv[:, nope:].T
        for i in range(n_blk):
            kl = (i + 1) * QBLK
            st = scores(h, i)
            top = jnp.max(st, axis=0, keepdims=True)
            pt = jnp.exp(st - top)
            total = jnp.sum(pt, axis=0, keepdims=True)
            ot = mm(vt_s[:, :kl], pt.astype(BF16)) * (1.0 / total)
            ot_st[pl.ds(pl.multiple_of(h * nope, nope), nope), i * QBLK:kl] = ot.astype(BF16)
            lse_s[h, :, i * QBLK:kl] = top + jnp.log(total)
        return carry
    lax.fori_loop(0, heads, forward, 0)

    ot_dst = ot_out.at[pl.ds(pl.multiple_of(core * heads * nope, heads * nope), heads * nope), :]
    ot_local = pltpu.make_async_copy(ot_st, ot_dst, kr_sem.at[3])
    ot_remote = pltpu.make_async_remote_copy(src_ref=ot_st, dst_ref=ot_dst, send_sem=kr_sem.at[4], recv_sem=kr_sem.at[5], device_id={'cp': partner}, device_id_type=mesh_id)
    ot_local.start()
    ot_remote.start()
    for rel in range(n_chips):
        for p in range(PARTS):
            across(1, rel, p).wait_recv()
    outs[3].start()
    outs[2].wait()
    c_s[...] = jnp.zeros_like(c_s)

    def head_copies(step, hh):
        slot_of = lax.rem(step, 2)
        head = (core * n_pairs + step) * 2 + hh
        col = pl.ds(pl.multiple_of(head * nope, nope), nope)
        cols = pl.ds(hh * nope, nope)
        regions = ((dqt_st.at[slot_of, pl.ds(hh * qk, qk), :], dqt_out.at[pl.ds(pl.multiple_of(head * qk, qk), qk), :]), (dk_st.at[slot_of, :, cols], dk_out.at[:, col]), (dv_st.at[slot_of, :, cols], dv_out.at[:, col]))
        local, remote = [], []
        for idx, (src, dst) in enumerate(regions):
            local.append(pltpu.make_async_copy(src, dst, loc_sem.at[slot_of, hh, idx]))
            remote.append(pltpu.make_async_remote_copy(src_ref=src, dst_ref=dst, send_sem=snd_sem.at[slot_of, hh, idx], recv_sem=rcv_sem.at[step, hh, idx], device_id={'cp': partner}, device_id_type=mesh_id))
        return local, remote

    theirs = pl.ds(pl.multiple_of((1 - core) * rows, rows), rows)
    mine = pl.ds(pl.multiple_of(core * rows, rows), rows)
    sums = [pltpu.make_async_remote_copy(src_ref=acc.at[theirs, :], dst_ref=buf, send_sem=yx_sem.at[idx], recv_sem=yx_sem.at[2 + idx], device_id={'cp': partner}, device_id_type=mesh_id) for idx, (acc, buf) in enumerate(((y_acc, y_buf), (dx_acc, dx_buf)))]
    chip_cols = pl.ds(pl.multiple_of(chip * both, both), both)

    def backward(g, carry):
        slot = lax.rem(g, 2)

        @pl.when(g >= 2)
        def _():
            for hh in range(2):
                local, remote = head_copies(g - 2, hh)
                for copy in local:
                    copy.wait()
                for copy in remote:
                    copy.wait_send()
        wo_copy(g).wait()
        do_all = mm(gy_s[...], wo_s[slot], NT).astype(BF16)
        do_s[...] = do_all
        dot_s[...] = do_all.T
        y_acc[...] += mm(ot_st[pl.ds(pl.multiple_of(g * 2 * nope, 2 * nope), 2 * nope), chip_cols], wo_s[slot], TN)

        @pl.when(g == n_pairs - 1)
        def _():
            sums[0].start()
        for hh in range(2):
            h = 2 * g + hh
            cols = slice(hh * nope, (hh + 1) * nope)
            for i in range(n_blk):
                kl = (i + 1) * QBLK
                lo = i * QBLK
                blk = slice(lo, kl)
                pt = jnp.exp(scores(h, i) - lse_s[h, :, blk])
                dpt = mm(v_s[h, :kl, :], dot_s[cols, blk])
                pdp = pt * dpt
                row_dot = jnp.sum(pdp, axis=0, keepdims=True)
                dst = ((pdp - pt * row_dot) * scale).astype(BF16)
                dv_add = mm(pt.astype(BF16), do_s[blk, cols])
                dk_add = mm(dst, q_s[h, blk, :])
                if i:
                    dv_acc[:lo, :] += dv_add[:lo, :]
                    dk_acc[:lo, :] += dk_add[:lo, :]
                dv_acc[blk, :] = dv_add[lo:, :]
                dk_acc[blk, :] = dk_add[lo:, :]
                kt_blk = jnp.concatenate([kt_s[h, :, :kl], krt_s[:, :kl]], axis=0)
                dqt = mm(kt_blk, dst)
                r1 = dqt[nope:nope + half, :]
                r2 = dqt[nope + half:nope + rope_dim, :]
                c_t = tabt_s[:half, blk]
                s_t = tabt_s[LANES - half:, blk]
                dqt_rot = jnp.concatenate([dqt[:nope, :], r1 * c_t + r2 * s_t, r2 * c_t - r1 * s_t], axis=0)
                dqt_st[slot, hh * qk:(hh + 1) * qk, blk] = dqt_rot.astype(BF16)
            dk_st[slot, :, cols] = dk_acc[:, :nope].astype(BF16)
            dv_st[slot, :, cols] = dv_acc[...].astype(BF16)
            local, remote = head_copies(g, hh)
            for copy in remote + local:
                copy.start()
            dkv = jnp.concatenate([dk_st[slot, :, cols], dv_st[slot, :, cols]], axis=1)
            c_s[...] += mm(dkv, wkv_s[h], NT)
            dkr_acc[...] += dk_acc[:, nope:]
            dx_acc[...] += mm(dqt_st[slot, hh * qk:(hh + 1) * qk, chip_cols], wq_s[h, :qk, :], TN)

        @pl.when(g + 2 < n_pairs)
        def _():
            wo_copy(g + 2).start()
        return carry
    lax.fori_loop(0, n_pairs, backward, 0)

    kr_local = pltpu.make_async_copy(dkr_acc, dkr_out.at[core], kr_sem.at[0])
    kr_remote = pltpu.make_async_remote_copy(src_ref=dkr_acc, dst_ref=dkr_out.at[core], send_sem=kr_sem.at[1], recv_sem=kr_sem.at[2], device_id={'cp': partner}, device_id_type=mesh_id)
    dlat_local = pltpu.make_async_copy(c_s, dlat_out.at[core], dlat_sem.at[0])
    dlat_remote = pltpu.make_async_remote_copy(src_ref=c_s, dst_ref=dlat_out.at[core], send_sem=dlat_sem.at[1], recv_sem=dlat_sem.at[2], device_id={'cp': partner}, device_id_type=mesh_id)
    for copy in (dlat_remote, sums[1], kr_remote, kr_local, dlat_local):
        copy.start()
    for arr in range(2):
        for p in range(PARTS):
            for d in range(2):
                for h in range(far if d == p // (PARTS // 2) else far - 1):
                    ring(arr, d, h, p, h == 0).wait_send()
            for rel in range(n_chips):
                across(arr, rel, p, rel == 0).wait_send()
    for copy in (outs[0], outs[1], outs[3]):
        copy.wait()
    ot_local.wait()
    ot_remote.wait()
    for step in range(n_pairs):
        for hh in range(2):
            local, remote = head_copies(step, hh)
            if step >= n_pairs - 2:
                for copy in local:
                    copy.wait()
                for copy in remote:
                    copy.wait_send()
            for copy in remote:
                copy.wait_recv()
    kr_local.wait()
    kr_remote.wait()
    dlat_local.wait()
    dlat_remote.wait()
    for copy in sums:
        copy.wait()
    y_out[...] = (y_acc[mine, :] + y_buf[...]).astype(BF16)
    dx_out[...] = dx_acc[mine, :] + dx_buf[...]


def block(x_loc, gy_loc, tab, wq_rows, w_dkv, g_row, wkr_t, w_uk, w_uv, wo_rows, n_dev, qk, scale):
    rows, width = x_loc.shape
    seq = rows * n_dev
    n_chips = n_dev // 2
    rank = w_dkv.shape[1]
    nope = LANES
    n_hv = wo_rows.shape[0]
    n_feat = wq_rows.shape[0]
    heads = n_hv // nope // 2
    n_pairs = heads // 2
    far = n_chips // 2
    hbm = pl.BlockSpec(memory_space=pl.ANY)
    vmem = pl.BlockSpec(memory_space=pltpu.VMEM)
    dma = pltpu.SemaphoreType.DMA
    vm = pltpu.VMEM
    sds = jax.ShapeDtypeStruct
    scratch = [vm((seq, width), BF16), vm((seq, width), BF16), vm((seq, LANES), F32), vm((LANES, seq), F32), vm((heads, 2 * LANES, width), BF16), vm((width, rank), BF16), vm((LANES, width), BF16),
               vm((2, rank, heads, nope), BF16), vm((rank * heads, nope), F32), vm((heads, rank, 2 * nope), BF16), vm((2, 2 * nope, width), BF16),
               vm((heads, seq, 2 * LANES), BF16), vm((seq, rank), BF16), vm((seq, rank), F32), vm((seq, LANES), BF16), vm((LANES, seq), BF16),
               vm((heads, seq, nope), BF16), vm((heads, seq, nope), BF16), vm((heads, nope, seq), BF16), vm((nope, seq), BF16), vm((heads, 1, seq), F32), vm((heads * nope, seq), BF16),
               vm((seq, 2 * nope), BF16), vm((2 * nope, seq), BF16), vm((seq, 2 * LANES), F32), vm((seq, nope), F32), vm((seq, LANES), F32),
               vm((2 * rows, width), F32), vm((2 * rows, width), F32), vm((rows, width), F32), vm((rows, width), F32),
               vm((2, 2 * qk, seq), BF16), vm((2, seq, 2 * nope), BF16), vm((2, seq, 2 * nope), BF16),
               dma((2, 2, far, PARTS)), dma((2, 2, far, PARTS)), dma((2, n_chips, PARTS)), dma((2, n_chips, PARTS)), dma((7,)), dma((heads,)), dma((2,)), dma((4,)), dma((2, 2, 3)), dma((2, 2, 3)), dma((n_pairs, 2, 3)), dma((6,)), dma((4,)), dma((3,))]
    return pl.pallas_call(
        functools.partial(block_kernel, n_chips, qk, scale),
        out_shape=(sds((seq, width), BF16), sds((seq, width), BF16), sds((seq, rank), BF16), sds((seq, rank), F32), sds((n_hv, seq), BF16), sds((n_feat, seq), BF16), sds((seq, n_hv), BF16), sds((seq, n_hv), BF16), sds((2, seq, LANES), F32), sds((2, seq, rank), F32), sds((rows, width), BF16), sds((rows, width), F32)),
        in_specs=[hbm] * 5 + [vmem] + [hbm] * 4,
        out_specs=[hbm] * 10 + [vmem] * 2,
        scratch_shapes=scratch,
        compiler_params=pltpu.CompilerParams(collective_id=0, has_side_effects=True, vmem_limit_bytes=67043328),
        name='latent_block',
    )(x_loc, gy_loc, tab, wq_rows, w_dkv, g_row, wkr_t, w_uk, w_uv, wo_rows)


def grads_kernel(tile, tile_c, chunk, rope_dim, ot_ref, dqt_ref, gy_ref, x_ref, lat_ref, dk_ref, dv_ref, dlat_ref, c_ref, dkr_ref, tab_ref, wdkv_ref, wkr_ref, dxq_ref, gkv_ref, gwo_ref, gwq_ref, guk_ref, guv_ref, gdkv_ref, gkr_ref, gg_ref, dx_ref,
                 lhs_s, rhs_s, lat_s, latt_s, kv_s, stage, stage_kv, dlat_s, c_s, dkr_s, tab_s, wdkv_s, wkr_s, dxq_s, side_s, sidet_s, dkv_st, in_sem, out_sem, kv_sem, dkv_sem):
    n_o, n_q = ot_ref.shape[0] // tile, dqt_ref.shape[0] // tile
    heads = kv_s.shape[2] // LANES
    rank = lat_s.shape[1]
    n_c = rank // tile_c
    rest = [(ot_ref.at[pl.ds(tile, (n_o - 1) * tile), :], lhs_s.at[pl.ds(tile, (n_o - 1) * tile), :]), (x_ref, rhs_s.at[1]), (dqt_ref, lhs_s.at[pl.ds(n_o * tile, n_q * tile), :]), (lat_ref, lat_s), (dk_ref, kv_s.at[0]), (dv_ref, kv_s.at[1]), (dlat_ref, dlat_s), (c_ref, c_s), (dkr_ref, dkr_s), (tab_ref, tab_s), (wdkv_ref, wdkv_s), (wkr_ref, wkr_s), (dxq_ref, dxq_s)]
    loads = [pltpu.make_async_copy(src, dst, in_sem.at[idx]) for idx, (src, dst) in enumerate([(ot_ref.at[pl.ds(0, tile), :], lhs_s.at[pl.ds(0, tile), :]), (gy_ref, rhs_s.at[0])] + rest)]
    for copy in loads:
        copy.start()

    def out_copy(t, dst, base):
        slot = lax.rem(t, 2)
        return pltpu.make_async_copy(stage.at[slot], dst.at[pl.ds(pl.multiple_of((t - base) * tile, tile), tile), :], out_sem.at[slot])

    loads[0].wait()
    loads[1].wait()

    def product(t, carry):
        slot = lax.rem(t, 2)

        @pl.when(t == 1)
        def _():
            loads[2].wait()

        @pl.when(t == n_o)
        def _():
            loads[3].wait()
            loads[4].wait()

        @pl.when(t >= 2)
        def _():
            out_copy(t, gwo_ref, t).wait()
        which = jnp.where(t < n_o, 0, 1)
        stage[slot] = mm(lhs_s[pl.ds(pl.multiple_of(t * tile, tile), tile), :], rhs_s[which])

        @pl.when(t < n_o)
        def _():
            out_copy(t, gwo_ref, 0).start()

        @pl.when(t >= n_o)
        def _():
            out_copy(t, gwq_ref, n_o).start()
        return carry
    lax.fori_loop(0, n_o + n_q, product, 0)
    for copy in loads[5:]:
        copy.wait()
    latt_s[...] = lat_s[...].T

    def kv_copy(t, dst, base):
        slot = lax.rem(t, 2)
        size = tile_c * heads
        return pltpu.make_async_copy(stage_kv.at[slot], dst.at[pl.ds(pl.multiple_of((t - base) * size, size), size), :], kv_sem.at[slot])

    def latent_side(t, carry):
        slot = lax.rem(t, 2)

        @pl.when(t >= 2)
        def _():
            kv_copy(t, guk_ref, t).wait()
        which = jnp.where(t < n_c, 0, 1)
        row = pl.multiple_of((t - which * n_c) * tile_c, tile_c)
        res = mm(latt_s[pl.ds(row, tile_c), :], kv_s[which])
        for h in range(heads):
            stage_kv[slot, pl.ds(h, tile_c, stride=heads), :] = res[:, h * LANES:(h + 1) * LANES]

        @pl.when(t < n_c)
        def _():
            kv_copy(t, guk_ref, 0).start()

        @pl.when(t >= n_c)
        def _():
            kv_copy(t, guv_ref, n_c).start()
        return carry
    lax.fori_loop(0, 2 * n_c, latent_side, 0)

    c_raw = c_s[...]
    inv_rms = lax.rsqrt(jnp.mean(c_raw * c_raw, axis=-1, keepdims=True) + NORM_EPS)
    c_norm = c_raw * inv_rms
    d_lat = dlat_s[0] + dlat_s[1]
    gg_ref[...] = jnp.sum(d_lat * c_norm, axis=0, keepdims=True)
    d_norm = d_lat * gkv_ref[...]
    side_s[:, :rank] = (inv_rms * (d_norm - c_norm * jnp.mean(d_norm * c_norm, axis=-1, keepdims=True))).astype(BF16)
    d_kr = dkr_s[0] + dkr_s[1]
    tab = tab_s[...]
    lane = lax.broadcasted_iota(jnp.int32, tab.shape, 1)
    cos_v = jnp.where(lane < rope_dim, tab, 0.0)
    sin_v = jnp.where(lane < rope_dim, pltpu.roll(tab, rope_dim, 1), 0.0)
    side_s[:, rank:] = (d_kr * cos_v - swap_halves(d_kr, rope_dim // 2) * sin_v).astype(BF16)
    sidet_s[...] = side_s[...].T

    def dkv_copy(t):
        slot = lax.rem(t, 2)
        return pltpu.make_async_copy(dkv_st.at[slot], gdkv_ref.at[pl.ds(pl.multiple_of(t * chunk, chunk), chunk), :], dkv_sem.at[slot])

    def side(t, carry):
        slot = lax.rem(t, 2)

        @pl.when(t >= 2)
        def _():
            dkv_copy(t - 2).wait()
        cols = pl.ds(pl.multiple_of(t * chunk, chunk), chunk)
        res = mm(sidet_s[...], rhs_s[1, :, cols])
        dkv_st[slot] = res[:rank, :].T
        gkr_ref[:, cols] = res[rank:rank + rope_dim, :]
        dkv_copy(t).start()
        return carry
    n_chunks = rhs_s.shape[2] // chunk
    lax.fori_loop(0, n_chunks, side, 0)
    rows = dxq_s.shape[0]
    own = pl.ds(pl.multiple_of(lax.axis_index('cp') * rows, rows), rows)
    dx_ref[...] = (dxq_s[...] + mm(side_s[own, :rank], wdkv_s[...], NT) + mm(side_s[own, rank:rank + rope_dim], wkr_s[...])).astype(BF16)
    for t in range(n_chunks - 2, n_chunks):
        dkv_copy(t).wait()
    for t in range(2):
        out_copy(t, gwo_ref, t).wait()
        kv_copy(t, guk_ref, t).wait()


def big_grads(o_t, dq_t, gy_all, x_all, latent, dk, dv, dlat, c_raw, dkr, tab, w_dkv, wkr_t, dx_q, g_row):
    tile, tile_c, chunk = 512, 256, 512
    seq, width = x_all.shape
    n_hv, n_feat, rank = o_t.shape[0], dq_t.shape[0], latent.shape[1]
    heads = n_hv // LANES
    rows = dx_q.shape[0]
    rope_dim = wkr_t.shape[0]
    hbm = pl.BlockSpec(memory_space=pl.ANY)
    vmem = pl.BlockSpec(memory_space=pltpu.VMEM)
    dma = pltpu.SemaphoreType.DMA
    vm = pltpu.VMEM
    sds = jax.ShapeDtypeStruct
    flops = 2 * seq * width * (n_hv + n_feat + rank) + 4 * seq * rank * n_hv
    return pl.pallas_call(
        functools.partial(grads_kernel, tile, tile_c, chunk, rope_dim),
        out_shape=(sds((n_hv, width), F32), sds((n_feat, width), F32), sds((rank * heads, LANES), F32), sds((rank * heads, LANES), F32), sds((width, rank), F32), sds((rope_dim, width), F32), sds((1, rank), F32), sds((rows, width), BF16)),
        in_specs=[hbm] * 14 + [vmem],
        out_specs=[hbm] * 5 + [vmem] * 3,
        scratch_shapes=[vm((n_hv + n_feat, seq), BF16), vm((2, seq, width), BF16), vm((seq, rank), BF16), vm((rank, seq), BF16), vm((2, seq, n_hv), BF16), vm((2, tile, width), F32), vm((2, tile_c * heads, LANES), F32),
                        vm((2, seq, rank), F32), vm((seq, rank), F32), vm((2, seq, LANES), F32), vm((seq, LANES), F32), vm((width, rank), BF16), vm((rope_dim, width), BF16), vm((rows, width), F32), vm((seq, rank + LANES), BF16), vm((rank + LANES, seq), BF16), vm((2, chunk, rank), F32),
                        dma((15,)), dma((2,)), dma((2,)), dma((2,))],
        compiler_params=pltpu.CompilerParams(vmem_limit_bytes=67043328),
        cost_estimate=pl.CostEstimate(flops=flops, bytes_accessed=90 * 1024 * 1024, transcendentals=0),
        name='weight_grads',
    )(o_t, dq_t, gy_all, x_all, latent, dk, dv, dlat, c_raw, dkr, tab, w_dkv, wkr_t, dx_q, g_row)


def solution(mesh):
    n_dev = mesh.shape['cp']
    row_spec = P(('dp', 'cp'), None)
    in_specs = (row_spec, row_spec, P(), P(), P(), P(), P(), P(), P())
    out_specs = (row_spec, row_spec, P('dp', None, None), P('dp', None), P('dp'), P('dp', None), P('dp', None, None), P('dp', None, None), P('dp', None, None))

    def device_fn(x_loc, gy_loc, w_q, w_dkv, g_kv, w_kr, w_uk, w_uv, w_o):
        rows, width = x_loc.shape
        seq = rows * n_dev
        heads, qk = w_q.shape[1:]
        rope_dim = w_kr.shape[1]
        rank = w_dkv.shape[1]
        nope = qk - rope_dim
        scale = qk ** -0.5
        half = rope_dim // 2
        inv_freq = ROPE_THETA ** (-(np.arange(half) * 2.0 / rope_dim))
        angles = np.arange(seq)[:, None] * inv_freq[None, :]
        cos, sin = np.cos(angles).astype(np.float32), np.sin(angles).astype(np.float32)
        tab = jnp.asarray(np.concatenate([cos, cos, -sin, sin], axis=1))

        wq_rows = jnp.transpose(w_q, (1, 2, 0)).reshape(heads * qk, width)
        wo_rows = w_o.reshape(heads * nope, width)
        g_f32 = g_kv.astype(F32)
        g_row = g_f32[None, :]
        wkr_t = w_kr.T
        x_all, gy_all, latent, c_raw, o_t, dq_t, dk, dv, dkr, dlat, y_loc, dx_q = block(x_loc, gy_loc, tab, wq_rows, w_dkv, g_row, wkr_t, w_uk, w_uv, wo_rows, n_dev, qk, scale)
        gwo, gwq, guk, guv, gw_dkv, gkr_t, gg, dx_loc = big_grads(o_t, dq_t, gy_all, x_all, latent, dk, dv, dlat, c_raw, dkr, tab, w_dkv, wkr_t, dx_q, g_row)
        gw_q = jnp.transpose(gwq.reshape(heads, qk, width), (2, 0, 1))
        return (y_loc, dx_loc, gw_q, gw_dkv, gg.reshape(rank), gkr_t.T, guk.reshape(w_uk.shape), guv.reshape(w_uv.shape), gwo.reshape(w_o.shape))

    return jax.shard_map(device_fn, mesh=mesh, in_specs=in_specs, out_specs=out_specs, check_vma=False)
```

```python
import functools

import jax
import jax.numpy as jnp
import numpy as np
from jax import lax
from jax.experimental import pallas as pl
from jax.experimental.pallas import tpu as pltpu
from jax.sharding import PartitionSpec as P

ROPE_THETA = 10000.0
NORM_EPS = 1e-6
QBLK = 256
MASKED = -1e30
LANES = 128
PARTS = 4
F32 = jnp.float32
BF16 = jnp.bfloat16
NN = (((1,), (0,)), ((), ()))
NT = (((1,), (1,)), ((), ()))
TN = (((0,), (0,)), ((), ()))


def mm(lhs, rhs, dims=NN):
    return lax.dot_general(lhs, rhs, dims, preferred_element_type=F32)


def swap_halves(t, half):
    return pltpu.roll(t, half, 1) + pltpu.roll(t, LANES - half, 1)


def block_kernel(n_chips, qk, scale, x_ref, gy_ref, tab_ref, wq_ref, wdkv_ref, gkv_ref, wkr_ref, wuk_ref, wuv_ref, wo_ref,
                 x_out, gy_out, lat_out, c_out, ot_out, dqt_out, dk_out, dv_out, dkr_out, dlat_out, y_out, dx_out,
                 x_s, gy_s, tab_s, tabt_s, wq_s, wdkv_s, wkr_s, wkv_raw, wkv_f32, wkv_s, wo_s, q_s, lat_s, c_s, kr_s, krt_s,
                 kn_s, v_s, kt_s, vt_s, lse_s, ot_st, do_s, dot_s, dk_acc, dv_acc, dkr_acc, y_acc, dx_acc, y_buf, dx_buf,
                 dqt_st, dk_st, dv_st,
                 ring_send, ring_recv, pr_send, pr_recv, w_sem, wq_sem, wo_sem, out_sem, loc_sem, snd_sem, rcv_sem, kr_sem, yx_sem, dlat_sem):
    me = lax.axis_index('cp')
    core = lax.rem(me, 2)
    chip = lax.div(me, 2)
    partner = me + 1 - 2 * core
    ring_dev = (lax.rem(chip + 1, n_chips) * 2 + core, lax.rem(chip + n_chips - 1, n_chips) * 2 + core)
    rows = x_ref.shape[0]
    part = rows // PARTS
    both = 2 * rows
    seq = x_s.shape[0]
    heads = wq_s.shape[0]
    n_pairs = heads // 2
    nope = LANES
    rope_dim = wkr_ref.shape[0]
    half = rope_dim // 2
    far = n_chips // 2
    mesh_id = pl.DeviceIdType.MESH
    srcs, bufs = (x_ref, gy_ref), (x_s, gy_s)

    def origin(d, h):
        return lax.rem(chip + (n_chips - h if d == 0 else h), n_chips)

    def piece(arr, chip_of, core_of, p):
        start = pl.multiple_of((chip_of * 2 + core_of) * rows + p * part, part)
        return bufs[arr].at[pl.ds(start, part), :]

    def ring(arr, d, h, p, first=False):
        dst = piece(arr, origin(d, h), core, p)
        src = srcs[arr].at[pl.ds(p * part, part), :] if first else dst
        return pltpu.make_async_remote_copy(src_ref=src, dst_ref=dst, send_sem=ring_send.at[arr, d, h, p], recv_sem=ring_recv.at[arr, d, h, p], device_id={'cp': ring_dev[d]}, device_id_type=mesh_id)

    def across(arr, rel, p, first=False):
        dst = piece(arr, lax.rem(chip + n_chips - rel, n_chips), core, p)
        src = srcs[arr].at[pl.ds(p * part, part), :] if first else dst
        return pltpu.make_async_remote_copy(src_ref=src, dst_ref=dst, send_sem=pr_send.at[arr, rel, p], recv_sem=pr_recv.at[arr, rel, p], device_id={'cp': partner}, device_id_type=mesh_id)

    def hop(arr, h, p):
        for d in range(2):
            limit = jnp.where(lax.div(p, PARTS // 2) == d, far, far - 1)

            @pl.when(h <= limit)
            def _():
                ring(arr, d, h - 1, p).wait_recv()

                @pl.when(h < limit)
                def _():
                    ring(arr, d, h, p).start()
                across(arr, h if d == 0 else n_chips - h, p).start()

    def weight_copies():
        first = core * heads
        out = [pltpu.make_async_copy(wuk_ref.at[:, pl.ds(pl.multiple_of(first, heads), heads), :], wkv_raw.at[0], w_sem.at[2]),
               pltpu.make_async_copy(wuv_ref.at[:, pl.ds(pl.multiple_of(first, heads), heads), :], wkv_raw.at[1], w_sem.at[3]),
               pltpu.make_async_copy(wkr_ref, wkr_s.at[pl.ds(0, rope_dim), :], w_sem.at[1]),
               pltpu.make_async_copy(tab_ref, tab_s, w_sem.at[4]),
               pltpu.make_async_copy(wdkv_ref, wdkv_s, w_sem.at[0])]
        for idx in range(2):
            out.append(pltpu.make_async_copy(srcs[idx], bufs[idx].at[pl.ds(pl.multiple_of(me * rows, rows), rows), :], w_sem.at[5 + idx]))
        for hh in range(heads):
            start = pl.multiple_of((first + hh) * qk, qk)
            out.append(pltpu.make_async_copy(wq_ref.at[pl.ds(start, qk), :], wq_s.at[hh, pl.ds(0, qk), :], wq_sem.at[hh]))
        return out

    def wo_copy(step):
        start = pl.multiple_of((core * n_pairs + step) * 2 * nope, 2 * nope)
        slot = lax.rem(step, 2)
        return pltpu.make_async_copy(wo_ref.at[pl.ds(start, 2 * nope), :], wo_s.at[slot], wo_sem.at[slot])

    barrier = pltpu.get_barrier_semaphore()
    for peer in (ring_dev[0], ring_dev[1], partner):
        pl.semaphore_signal(barrier, inc=1, device_id={'cp': peer}, device_id_type=mesh_id)
    pl.semaphore_wait(barrier, 3)
    for p in range(PARTS):
        for d in range(2):
            ring(0, d, 0, p, True).start()
    for arr in range(2):
        for p in range(PARTS):
            across(arr, 0, p, True).start()
    for copy in weight_copies():
        copy.start()
    wo_copy(0).start()
    wo_copy(1).start()

    weights = weight_copies()
    rank = wkv_raw.shape[1]
    for p in range(PARTS):
        hop(0, 1, p)
        if p == 0:
            wq_s[:, qk:, :] = jnp.zeros((heads, 2 * LANES - qk, wq_s.shape[2]), BF16)
            wkr_s[rope_dim:, :] = jnp.zeros((LANES - rope_dim, wkr_s.shape[1]), BF16)
            dkr_acc[...] = jnp.zeros_like(dkr_acc)
            y_acc[...] = jnp.zeros_like(y_acc)
            dx_acc[...] = jnp.zeros_like(dx_acc)
        elif p <= 2:
            idx = p - 1
            weights[idx].wait()
            wkv_f32[...] = wkv_raw[idx].astype(F32).reshape(rank * heads, LANES)
            for hh in range(heads):
                wkv_s[hh, :, idx * nope:(idx + 1) * nope] = wkv_f32[pl.ds(hh, rank, stride=heads), :].astype(BF16)
    for copy in weights[2:]:
        copy.wait()
    tabt_s[...] = tab_s[...].T

    lane = lax.broadcasted_iota(jnp.int32, (2 * both, LANES), 1)

    def x_stage(h, carry):
        near = h - 1
        up_rel = near
        dn_rel = jnp.where(near < far, n_chips - near, 0)
        chips = (lax.rem(chip + n_chips - up_rel, n_chips), lax.rem(chip + n_chips - dn_rel, n_chips))
        starts = [pl.multiple_of(c * both, both) for c in chips]

        def rows_of(ref):
            return jnp.concatenate([ref[pl.ds(st, both), :] for st in starts], axis=0)

        def put(ref, val):
            for idx, st in enumerate(starts):
                ref[pl.ds(st, both), :] = val[idx * both:(idx + 1) * both, :]

        def rotate(t):
            tab = rows_of(tab_s)
            cos_v = jnp.where(lane < rope_dim, tab, 0.0)
            sin_v = jnp.where(lane < rope_dim, pltpu.roll(tab, rope_dim, 1), 0.0)
            return (t * cos_v + swap_halves(t, half) * sin_v).astype(BF16)

        def quarter(j, carry):
            @pl.when(h <= far)
            def _():
                hop(0, h, j)

            @pl.when(h > far)
            def _():
                hop(1, 1, j)

            @pl.when((h == far - 1) & (j == PARTS - 1))
            def _():
                for p in range(PARTS):
                    for d in range(2):
                        ring(1, d, 0, p, True).start()

            @pl.when(j == 0)
            def _():
                for p in range(PARTS):
                    across(0, up_rel, p).wait_recv()
                    across(0, dn_rel, p).wait_recv()
                x_blk = rows_of(x_s)
                c_raw = mm(x_blk, wdkv_s[...])
                put(c_s, c_raw)
                inv_rms = lax.rsqrt(jnp.mean(c_raw * c_raw, axis=-1, keepdims=True) + NORM_EPS)
                put(lat_s, (c_raw * inv_rms * gkv_ref[...]).astype(BF16))
                put(kr_s, rotate(mm(x_blk, wkr_s[...], NT)))
            x_blk = rows_of(x_s)
            for hh in range(heads // PARTS):
                head = j * (heads // PARTS) + hh
                q_raw = mm(x_blk, wq_s[head], NT)
                q_val = jnp.concatenate([q_raw[:, :nope].astype(BF16), rotate(q_raw[:, nope:])], axis=1)
                for idx, st in enumerate(starts):
                    q_s[head, pl.ds(st, both), :] = q_val[idx * both:(idx + 1) * both, :]
            return carry
        lax.fori_loop(0, PARTS, quarter, 0)
        return carry

    lax.fori_loop(2, far + 2, x_stage, 0)

    outs = [pltpu.make_async_copy(src, dst, out_sem.at[idx]) for idx, (src, dst) in enumerate(((x_s, x_out), (lat_s, lat_out), (c_s, c_out), (gy_s, gy_out)))]
    for copy in outs[:3]:
        copy.start()
    krt_s[...] = kr_s[...].T

    row_id = lax.broadcasted_iota(jnp.int32, (QBLK, QBLK), 0)
    col_id = lax.broadcasted_iota(jnp.int32, (QBLK, QBLK), 1)
    causal = row_id <= col_id
    n_blk = seq // QBLK

    def scores(h, i):
        kl = (i + 1) * QBLK
        k_blk = jnp.concatenate([kn_s[h, :kl, :], kr_s[:kl, :]], axis=1)
        st = mm(k_blk, q_s[h, i * QBLK:kl, :], NT) * scale
        diag = jnp.where(causal, st[i * QBLK:, :], MASKED)
        return diag if i == 0 else jnp.concatenate([st[:i * QBLK, :], diag], axis=0)

    def forward(h, carry):
        point = jnp.where(h < heads // 2, 2 * h, h + heads // 2)
        hop(1, 2 + lax.div(point, PARTS), lax.rem(point, PARTS))

        @pl.when(h < heads // 2)
        def _():
            hop(1, 2 + lax.div(point + 1, PARTS), lax.rem(point + 1, PARTS))
        kv = mm(lat_s[...], wkv_s[h]).astype(BF16)
        kn_s[h] = kv[:, :nope]
        v_s[h] = kv[:, nope:]
        kt_s[h] = kv[:, :nope].T
        vt_s[...] = kv[:, nope:].T
        for i in range(n_blk):
            kl = (i + 1) * QBLK
            st = scores(h, i)
            top = jnp.max(st, axis=0, keepdims=True)
            pt = jnp.exp(st - top)
            total = jnp.sum(pt, axis=0, keepdims=True)
            ot = mm(vt_s[:, :kl], pt.astype(BF16)) * (1.0 / total)
            ot_st[pl.ds(pl.multiple_of(h * nope, nope), nope), i * QBLK:kl] = ot.astype(BF16)
            lse_s[h, :, i * QBLK:kl] = top + jnp.log(total)
        return carry
    lax.fori_loop(0, heads, forward, 0)

    ot_dst = ot_out.at[pl.ds(pl.multiple_of(core * heads * nope, heads * nope), heads * nope), :]
    ot_local = pltpu.make_async_copy(ot_st, ot_dst, kr_sem.at[3])
    ot_remote = pltpu.make_async_remote_copy(src_ref=ot_st, dst_ref=ot_dst, send_sem=kr_sem.at[4], recv_sem=kr_sem.at[5], device_id={'cp': partner}, device_id_type=mesh_id)
    ot_local.start()
    ot_remote.start()
    for rel in range(n_chips):
        for p in range(PARTS):
            across(1, rel, p).wait_recv()
    outs[3].start()
    outs[2].wait()
    c_s[...] = jnp.zeros_like(c_s)

    def head_copies(step, hh):
        slot_of = lax.rem(step, 2)
        head = (core * n_pairs + step) * 2 + hh
        col = pl.ds(pl.multiple_of(head * nope, nope), nope)
        cols = pl.ds(hh * nope, nope)
        regions = ((dqt_st.at[slot_of, pl.ds(hh * qk, qk), :], dqt_out.at[pl.ds(pl.multiple_of(head * qk, qk), qk), :]), (dk_st.at[slot_of, :, cols], dk_out.at[:, col]), (dv_st.at[slot_of, :, cols], dv_out.at[:, col]))
        local, remote = [], []
        for idx, (src, dst) in enumerate(regions):
            local.append(pltpu.make_async_copy(src, dst, loc_sem.at[slot_of, hh, idx]))
            remote.append(pltpu.make_async_remote_copy(src_ref=src, dst_ref=dst, send_sem=snd_sem.at[slot_of, hh, idx], recv_sem=rcv_sem.at[step, hh, idx], device_id={'cp': partner}, device_id_type=mesh_id))
        return local, remote

    theirs = pl.ds(pl.multiple_of((1 - core) * rows, rows), rows)
    mine = pl.ds(pl.multiple_of(core * rows, rows), rows)
    sums = [pltpu.make_async_remote_copy(src_ref=acc.at[theirs, :], dst_ref=buf, send_sem=yx_sem.at[idx], recv_sem=yx_sem.at[2 + idx], device_id={'cp': partner}, device_id_type=mesh_id) for idx, (acc, buf) in enumerate(((y_acc, y_buf), (dx_acc, dx_buf)))]
    chip_cols = pl.ds(pl.multiple_of(chip * both, both), both)

    def backward(g, carry):
        slot = lax.rem(g, 2)

        @pl.when(g >= 2)
        def _():
            for hh in range(2):
                local, remote = head_copies(g - 2, hh)
                for copy in local:
                    copy.wait()
                for copy in remote:
                    copy.wait_send()
        wo_copy(g).wait()
        do_all = mm(gy_s[...], wo_s[slot], NT).astype(BF16)
        do_s[...] = do_all
        dot_s[...] = do_all.T
        y_acc[...] += mm(ot_st[pl.ds(pl.multiple_of(g * 2 * nope, 2 * nope), 2 * nope), chip_cols], wo_s[slot], TN)

        @pl.when(g == n_pairs - 1)
        def _():
            sums[0].start()
        for hh in range(2):
            h = 2 * g + hh
            cols = slice(hh * nope, (hh + 1) * nope)
            for i in range(n_blk):
                kl = (i + 1) * QBLK
                lo = i * QBLK
                blk = slice(lo, kl)
                pt = jnp.exp(scores(h, i) - lse_s[h, :, blk])
                dpt = mm(v_s[h, :kl, :], dot_s[cols, blk])
                pdp = pt * dpt
                row_dot = jnp.sum(pdp, axis=0, keepdims=True)
                dst = ((pdp - pt * row_dot) * scale).astype(BF16)
                dv_add = mm(pt.astype(BF16), do_s[blk, cols])
                dk_add = mm(dst, q_s[h, blk, :])
                if i:
                    dv_acc[:lo, :] += dv_add[:lo, :]
                    dk_acc[:lo, :] += dk_add[:lo, :]
                dv_acc[blk, :] = dv_add[lo:, :]
                dk_acc[blk, :] = dk_add[lo:, :]
                kt_blk = jnp.concatenate([kt_s[h, :, :kl], krt_s[:, :kl]], axis=0)
                dqt = mm(kt_blk, dst)
                r1 = dqt[nope:nope + half, :]
                r2 = dqt[nope + half:nope + rope_dim, :]
                c_t = tabt_s[:half, blk]
                s_t = tabt_s[LANES - half:, blk]
                dqt_rot = jnp.concatenate([dqt[:nope, :], r1 * c_t + r2 * s_t, r2 * c_t - r1 * s_t], axis=0)
                dqt_st[slot, hh * qk:(hh + 1) * qk, blk] = dqt_rot.astype(BF16)
            dk_st[slot, :, cols] = dk_acc[:, :nope].astype(BF16)
            dv_st[slot, :, cols] = dv_acc[...].astype(BF16)
            local, remote = head_copies(g, hh)
            for copy in remote + local:
                copy.start()
            dkv = jnp.concatenate([dk_st[slot, :, cols], dv_st[slot, :, cols]], axis=1)
            c_s[...] += mm(dkv, wkv_s[h], NT)
            dkr_acc[...] += dk_acc[:, nope:]
            dx_acc[...] += mm(dqt_st[slot, hh * qk:(hh + 1) * qk, chip_cols], wq_s[h, :qk, :], TN)

        @pl.when(g + 2 < n_pairs)
        def _():
            wo_copy(g + 2).start()
        return carry
    lax.fori_loop(0, n_pairs, backward, 0)

    kr_local = pltpu.make_async_copy(dkr_acc, dkr_out.at[core], kr_sem.at[0])
    kr_remote = pltpu.make_async_remote_copy(src_ref=dkr_acc, dst_ref=dkr_out.at[core], send_sem=kr_sem.at[1], recv_sem=kr_sem.at[2], device_id={'cp': partner}, device_id_type=mesh_id)
    dlat_local = pltpu.make_async_copy(c_s, dlat_out.at[core], dlat_sem.at[0])
    dlat_remote = pltpu.make_async_remote_copy(src_ref=c_s, dst_ref=dlat_out.at[core], send_sem=dlat_sem.at[1], recv_sem=dlat_sem.at[2], device_id={'cp': partner}, device_id_type=mesh_id)
    for copy in (dlat_remote, sums[1], kr_remote, kr_local, dlat_local):
        copy.start()
    for arr in range(2):
        for p in range(PARTS):
            for d in range(2):
                for h in range(far if d == p // (PARTS // 2) else far - 1):
                    ring(arr, d, h, p, h == 0).wait_send()
            for rel in range(n_chips):
                across(arr, rel, p, rel == 0).wait_send()
    for copy in (outs[0], outs[1], outs[3]):
        copy.wait()
    ot_local.wait()
    ot_remote.wait()
    for step in range(n_pairs):
        for hh in range(2):
            local, remote = head_copies(step, hh)
            if step >= n_pairs - 2:
                for copy in local:
                    copy.wait()
                for copy in remote:
                    copy.wait_send()
            for copy in remote:
                copy.wait_recv()
    kr_local.wait()
    kr_remote.wait()
    dlat_local.wait()
    dlat_remote.wait()
    for copy in sums:
        copy.wait()
    y_out[...] = (y_acc[mine, :] + y_buf[...]).astype(BF16)
    dx_out[...] = dx_acc[mine, :] + dx_buf[...]


def block(x_loc, gy_loc, tab, wq_rows, w_dkv, g_row, wkr_t, w_uk, w_uv, wo_rows, n_dev, qk, scale):
    rows, width = x_loc.shape
    seq = rows * n_dev
    n_chips = n_dev // 2
    rank = w_dkv.shape[1]
    nope = LANES
    n_hv = wo_rows.shape[0]
    n_feat = wq_rows.shape[0]
    heads = n_hv // nope // 2
    n_pairs = heads // 2
    far = n_chips // 2
    hbm = pl.BlockSpec(memory_space=pl.ANY)
    vmem = pl.BlockSpec(memory_space=pltpu.VMEM)
    dma = pltpu.SemaphoreType.DMA
    vm = pltpu.VMEM
    sds = jax.ShapeDtypeStruct
    scratch = [vm((seq, width), BF16), vm((seq, width), BF16), vm((seq, LANES), F32), vm((LANES, seq), F32), vm((heads, 2 * LANES, width), BF16), vm((width, rank), BF16), vm((LANES, width), BF16),
               vm((2, rank, heads, nope), BF16), vm((rank * heads, nope), F32), vm((heads, rank, 2 * nope), BF16), vm((2, 2 * nope, width), BF16),
               vm((heads, seq, 2 * LANES), BF16), vm((seq, rank), BF16), vm((seq, rank), F32), vm((seq, LANES), BF16), vm((LANES, seq), BF16),
               vm((heads, seq, nope), BF16), vm((heads, seq, nope), BF16), vm((heads, nope, seq), BF16), vm((nope, seq), BF16), vm((heads, 1, seq), F32), vm((heads * nope, seq), BF16),
               vm((seq, 2 * nope), BF16), vm((2 * nope, seq), BF16), vm((seq, 2 * LANES), F32), vm((seq, nope), F32), vm((seq, LANES), F32),
               vm((2 * rows, width), F32), vm((2 * rows, width), F32), vm((rows, width), F32), vm((rows, width), F32),
               vm((2, 2 * qk, seq), BF16), vm((2, seq, 2 * nope), BF16), vm((2, seq, 2 * nope), BF16),
               dma((2, 2, far, PARTS)), dma((2, 2, far, PARTS)), dma((2, n_chips, PARTS)), dma((2, n_chips, PARTS)), dma((7,)), dma((heads,)), dma((2,)), dma((4,)), dma((2, 2, 3)), dma((2, 2, 3)), dma((n_pairs, 2, 3)), dma((6,)), dma((4,)), dma((3,))]
    return pl.pallas_call(
        functools.partial(block_kernel, n_chips, qk, scale),
        out_shape=(sds((seq, width), BF16), sds((seq, width), BF16), sds((seq, rank), BF16), sds((seq, rank), F32), sds((n_hv, seq), BF16), sds((n_feat, seq), BF16), sds((seq, n_hv), BF16), sds((seq, n_hv), BF16), sds((2, seq, LANES), F32), sds((2, seq, rank), F32), sds((rows, width), BF16), sds((rows, width), F32)),
        in_specs=[hbm] * 5 + [vmem] + [hbm] * 4,
        out_specs=[hbm] * 10 + [vmem] * 2,
        scratch_shapes=scratch,
        compiler_params=pltpu.CompilerParams(collective_id=0, has_side_effects=True, vmem_limit_bytes=67043328),
        name='latent_block',
    )(x_loc, gy_loc, tab, wq_rows, w_dkv, g_row, wkr_t, w_uk, w_uv, wo_rows)


def grads_kernel(tile, tile_c, chunk, rope_dim, ot_ref, dqt_ref, gy_ref, x_ref, lat_ref, dk_ref, dv_ref, dlat_ref, c_ref, dkr_ref, tab_ref, wdkv_ref, wkr_ref, dxq_ref, yin_ref, gkv_ref, gwo_ref, gwq_ref, guk_ref, guv_ref, gdkv_ref, y_ref, gkr_ref, gg_ref, dx_ref,
                 lhs_s, rhs_s, lat_s, latt_s, kv_s, stage, stage_kv, dlat_s, c_s, dkr_s, tab_s, wdkv_s, wkr_s, dxq_s, y_s, side_s, sidet_s, dkv_st, in_sem, out_sem, kv_sem, dkv_sem, y_sem):
    n_o, n_q = ot_ref.shape[0] // tile, dqt_ref.shape[0] // tile
    heads = kv_s.shape[2] // LANES
    rank = lat_s.shape[1]
    n_c = rank // tile_c
    rest = [(ot_ref.at[pl.ds(tile, (n_o - 1) * tile), :], lhs_s.at[pl.ds(tile, (n_o - 1) * tile), :]), (x_ref, rhs_s.at[1]), (dqt_ref, lhs_s.at[pl.ds(n_o * tile, n_q * tile), :]), (lat_ref, lat_s), (dk_ref, kv_s.at[0]), (dv_ref, kv_s.at[1]), (dlat_ref, dlat_s), (c_ref, c_s), (dkr_ref, dkr_s), (tab_ref, tab_s), (wdkv_ref, wdkv_s), (wkr_ref, wkr_s), (dxq_ref, dxq_s), (yin_ref, y_s)]
    loads = [pltpu.make_async_copy(src, dst, in_sem.at[idx]) for idx, (src, dst) in enumerate([(ot_ref.at[pl.ds(0, tile), :], lhs_s.at[pl.ds(0, tile), :]), (gy_ref, rhs_s.at[0])] + rest)]
    for copy in loads[:2]:
        copy.start()

    def out_copy(t, dst, base):
        slot = lax.rem(t, 2)
        return pltpu.make_async_copy(stage.at[slot], dst.at[pl.ds(pl.multiple_of((t - base) * tile, tile), tile), :], out_sem.at[slot])

    loads[0].wait()
    loads[1].wait()
    loads[2].start()

    def product(t, carry):
        slot = lax.rem(t, 2)

        @pl.when(t == 1)
        def _():
            loads[2].wait()
            for copy in loads[3:]:
                copy.start()

        @pl.when(t == n_o)
        def _():
            loads[3].wait()
            loads[4].wait()

        @pl.when(t >= 2)
        def _():
            out_copy(t, gwo_ref, t).wait()
        which = jnp.where(t < n_o, 0, 1)
        stage[slot] = mm(lhs_s[pl.ds(pl.multiple_of(t * tile, tile), tile), :], rhs_s[which])

        @pl.when(t < n_o)
        def _():
            out_copy(t, gwo_ref, 0).start()

        @pl.when(t >= n_o)
        def _():
            out_copy(t, gwq_ref, n_o).start()
        return carry
    lax.fori_loop(0, n_o + n_q, product, 0)
    for copy in loads[5:]:
        copy.wait()
    latt_s[...] = lat_s[...].T
    y_copy = pltpu.make_async_copy(y_s, y_ref, y_sem.at[0])
    y_copy.start()

    def kv_copy(t, dst, base):
        slot = lax.rem(t, 2)
        size = tile_c * heads
        return pltpu.make_async_copy(stage_kv.at[slot], dst.at[pl.ds(pl.multiple_of((t - base) * size, size), size), :], kv_sem.at[slot])

    def latent_side(t, carry):
        slot = lax.rem(t, 2)

        @pl.when(t >= 2)
        def _():
            kv_copy(t, guk_ref, t).wait()
        which = jnp.where(t < n_c, 0, 1)
        row = pl.multiple_of((t - which * n_c) * tile_c, tile_c)
        res = mm(latt_s[pl.ds(row, tile_c), :], kv_s[which])
        for h in range(heads):
            stage_kv[slot, pl.ds(h, tile_c, stride=heads), :] = res[:, h * LANES:(h + 1) * LANES]

        @pl.when(t < n_c)
        def _():
            kv_copy(t, guk_ref, 0).start()

        @pl.when(t >= n_c)
        def _():
            kv_copy(t, guv_ref, n_c).start()
        return carry
    lax.fori_loop(0, 2 * n_c, latent_side, 0)

    c_raw = c_s[...]
    inv_rms = lax.rsqrt(jnp.mean(c_raw * c_raw, axis=-1, keepdims=True) + NORM_EPS)
    c_norm = c_raw * inv_rms
    d_lat = dlat_s[0] + dlat_s[1]
    gg_ref[...] = jnp.sum(d_lat * c_norm, axis=0, keepdims=True)
    d_norm = d_lat * gkv_ref[...]
    side_s[:, :rank] = (inv_rms * (d_norm - c_norm * jnp.mean(d_norm * c_norm, axis=-1, keepdims=True))).astype(BF16)
    d_kr = dkr_s[0] + dkr_s[1]
    tab = tab_s[...]
    lane = lax.broadcasted_iota(jnp.int32, tab.shape, 1)
    cos_v = jnp.where(lane < rope_dim, tab, 0.0)
    sin_v = jnp.where(lane < rope_dim, pltpu.roll(tab, rope_dim, 1), 0.0)
    side_s[:, rank:] = (d_kr * cos_v - swap_halves(d_kr, rope_dim // 2) * sin_v).astype(BF16)
    sidet_s[...] = side_s[...].T

    def dkv_copy(t):
        slot = lax.rem(t, 2)
        return pltpu.make_async_copy(dkv_st.at[slot], gdkv_ref.at[pl.ds(pl.multiple_of(t * chunk, chunk), chunk), :], dkv_sem.at[slot])

    def side(t, carry):
        slot = lax.rem(t, 2)

        @pl.when(t >= 2)
        def _():
            dkv_copy(t - 2).wait()
        cols = pl.ds(pl.multiple_of(t * chunk, chunk), chunk)
        res = mm(sidet_s[...], rhs_s[1, :, cols])
        dkv_st[slot] = res[:rank, :].T
        gkr_ref[:, cols] = res[rank:rank + rope_dim, :]
        dkv_copy(t).start()
        return carry
    n_chunks = rhs_s.shape[2] // chunk
    lax.fori_loop(0, n_chunks, side, 0)
    rows = dxq_s.shape[0]
    own = pl.ds(pl.multiple_of(lax.axis_index('cp') * rows, rows), rows)
    dx_ref[...] = (dxq_s[...] + mm(side_s[own, :rank], wdkv_s[...], NT) + mm(side_s[own, rank:rank + rope_dim], wkr_s[...])).astype(BF16)
    for t in range(n_chunks - 2, n_chunks):
        dkv_copy(t).wait()
    y_copy.wait()
    for t in range(2):
        out_copy(t, gwo_ref, t).wait()
        kv_copy(t, guk_ref, t).wait()


def big_grads(o_t, dq_t, gy_all, x_all, latent, dk, dv, dlat, c_raw, dkr, tab, w_dkv, wkr_t, dx_q, y_in, g_row):
    tile, tile_c, chunk = 512, 256, 512
    seq, width = x_all.shape
    n_hv, n_feat, rank = o_t.shape[0], dq_t.shape[0], latent.shape[1]
    heads = n_hv // LANES
    rows = dx_q.shape[0]
    rope_dim = wkr_t.shape[0]
    hbm = pl.BlockSpec(memory_space=pl.ANY)
    vmem = pl.BlockSpec(memory_space=pltpu.VMEM)
    dma = pltpu.SemaphoreType.DMA
    vm = pltpu.VMEM
    sds = jax.ShapeDtypeStruct
    flops = 2 * seq * width * (n_hv + n_feat + rank) + 4 * seq * rank * n_hv
    return pl.pallas_call(
        functools.partial(grads_kernel, tile, tile_c, chunk, rope_dim),
        out_shape=(sds((n_hv, width), F32), sds((n_feat, width), F32), sds((rank * heads, LANES), F32), sds((rank * heads, LANES), F32), sds((width, rank), F32), sds((rows, width), BF16), sds((rope_dim, width), F32), sds((1, rank), F32), sds((rows, width), BF16)),
        in_specs=[hbm] * 15 + [vmem],
        out_specs=[hbm] * 6 + [vmem] * 3,
        scratch_shapes=[vm((n_hv + n_feat, seq), BF16), vm((2, seq, width), BF16), vm((seq, rank), BF16), vm((rank, seq), BF16), vm((2, seq, n_hv), BF16), vm((2, tile, width), F32), vm((2, tile_c * heads, LANES), F32),
                        vm((2, seq, rank), F32), vm((seq, rank), F32), vm((2, seq, LANES), F32), vm((seq, LANES), F32), vm((width, rank), BF16), vm((rope_dim, width), BF16), vm((rows, width), F32), vm((rows, width), BF16), vm((seq, rank + LANES), BF16), vm((rank + LANES, seq), BF16), vm((2, chunk, rank), F32),
                        dma((16,)), dma((2,)), dma((2,)), dma((2,)), dma((1,))],
        compiler_params=pltpu.CompilerParams(vmem_limit_bytes=67043328),
        cost_estimate=pl.CostEstimate(flops=flops, bytes_accessed=90 * 1024 * 1024, transcendentals=0),
        name='weight_grads',
    )(o_t, dq_t, gy_all, x_all, latent, dk, dv, dlat, c_raw, dkr, tab, w_dkv, wkr_t, dx_q, y_in, g_row)


def solution(mesh):
    n_dev = mesh.shape['cp']
    row_spec = P(('dp', 'cp'), None)
    in_specs = (row_spec, row_spec, P(), P(), P(), P(), P(), P(), P())
    out_specs = (row_spec, row_spec, P('dp', None, None), P('dp', None), P('dp'), P('dp', None), P('dp', None, None), P('dp', None, None), P('dp', None, None))

    def device_fn(x_loc, gy_loc, w_q, w_dkv, g_kv, w_kr, w_uk, w_uv, w_o):
        rows, width = x_loc.shape
        seq = rows * n_dev
        heads, qk = w_q.shape[1:]
        rope_dim = w_kr.shape[1]
        rank = w_dkv.shape[1]
        nope = qk - rope_dim
        scale = qk ** -0.5
        half = rope_dim // 2
        inv_freq = ROPE_THETA ** (-(np.arange(half) * 2.0 / rope_dim))
        angles = np.arange(seq)[:, None] * inv_freq[None, :]
        cos, sin = np.cos(angles).astype(np.float32), np.sin(angles).astype(np.float32)
        tab = jnp.asarray(np.concatenate([cos, cos, -sin, sin], axis=1))

        wq_rows = jnp.transpose(w_q, (1, 2, 0)).reshape(heads * qk, width)
        wo_rows = w_o.reshape(heads * nope, width)
        g_f32 = g_kv.astype(F32)
        g_row = g_f32[None, :]
        wkr_t = w_kr.T
        x_all, gy_all, latent, c_raw, o_t, dq_t, dk, dv, dkr, dlat, y_in, dx_q = block(x_loc, gy_loc, tab, wq_rows, w_dkv, g_row, wkr_t, w_uk, w_uv, wo_rows, n_dev, qk, scale)
        gwo, gwq, guk, guv, gw_dkv, y_loc, gkr_t, gg, dx_loc = big_grads(o_t, dq_t, gy_all, x_all, latent, dk, dv, dlat, c_raw, dkr, tab, w_dkv, wkr_t, dx_q, y_in, g_row)
        gw_q = jnp.transpose(gwq.reshape(heads, qk, width), (2, 0, 1))
        return (y_loc, dx_loc, gw_q, gw_dkv, gg.reshape(rank), gkr_t.T, guk.reshape(w_uk.shape), guv.reshape(w_uv.shape), gwo.reshape(w_o.shape))

    return jax.shard_map(device_fn, mesh=mesh, in_specs=in_specs, out_specs=out_specs, check_vma=False)
```
